32 devices in a mesh: kpt: 16 (over z, x, core), band: 2 (over y).
Axes of the slice: x: 2, y: 2, z: 4, core: 2. Of those that a mesh axis runs over, the one named last changes fastest.
Arguments:
- margins: bfloat16 [16, 12, 400, 800], P('kpt', None, 'band'), may hold values from -0.21875 to 0.21875
- subspace: bfloat16 [16, 400, 512], P('kpt', 'band'), may hold values from -6 to 6
- shell_weights: float32 [12], replicated, may hold values from 0.3 to 3
- window_count: int32 [16], P('kpt'), may hold values from 200 to 400
Outputs:
- new_subspace: float32 [16, 400, 512], P('kpt', 'band')
The draws below stay inside these ranges and needn't reach their ends.
Inputs may be any that keep to these rules, and one draw needn't show every extreme that they name: window_count[k] is the number of leading bands of k-point k inside its outer window; the other rows up to 400 are padding.
All inputs are finite; a program needn't handle non-finite values.
Results may differ from the reference program's by a relative error of at most 0.0025.
Values may be sent and summed in bfloat16 or wider, within the bound.
No kernel may reach another device: no remote copies, remote signals or barrier semaphores. Data moves between devices by JAX's collectives and lax.ppermute only.
A program may use at most 64 MiB of HBM per device.

```python
import math
import jax
import jax.numpy as jnp
import numpy as np
from jax import lax

NB = 400
NW = 256
NBV = 12
SWEEPS = 2
KX = 4
KY = 2
KZ = 2
K = 16


def plant(result, key, least, largest):
    dims = result.shape
    spot = [jax.random.randint(jax.random.fold_in(key, axis), (), 0, dims[axis]) for axis in range(len(dims))]
    result = result.at[tuple(spot)].set(least)
    longest = dims.index(max(dims))
    spot[longest] = (spot[longest] + 1) % dims[longest]
    return result.at[tuple(spot)].set(largest)


def levels(own_key, dims, split, smallest, high):
    def one(dim, parts):
        draws = jax.random.uniform(jax.random.fold_in(jax.random.fold_in(own_key, 6), dim), (parts,), jnp.float32, smallest / len(split), high / len(split))
        return jnp.repeat(jnp.exp(draws), dims[dim] // parts).reshape((-1,) + (1,) * (len(dims) - dim - 1))

    loudness = one(*split[0])
    for cut in split[1:]:
        loudness = loudness * one(*cut)
    return loudness


def gaussian(rng, dims, scale, most, pieces=(), kind=jnp.bfloat16):
    drawn = jax.random.normal(rng, dims, jnp.float32) * scale
    if len(pieces) > 0:
        drawn = levels(rng, dims, pieces, -0.22, 0.18) * drawn
    return jnp.clip(drawn, min=-most, max=most).astype(kind)


def setup_inputs(seed: int = 0) -> dict:
    splits = jax.random.split(jax.random.key(seed), 5)
    return {
        "margins": gaussian(splits[0], (K, NBV, NB, 2 * NB), (2 * NB) ** -0.5, 0.21875, ((0, 16), (2, 2))),
        "subspace": gaussian(splits[1], (K, NB, 2 * NW), 1.0, 6.0, ((0, 16), (1, 2))),
        "shell_weights": jnp.clip(jnp.exp(jax.random.uniform(splits[2], (NBV,), jnp.float32, math.log(0.3), math.log(3.0))), 0.3, 3.0),
        "window_count": plant(jax.random.randint(splits[3], (K,), NB // 2, NB + 1), jax.random.fold_in(splits[3], 1), NB // 2, NB).astype(jnp.int32),
    }


SHELL_VECTORS = ((1, 1, 0), (1, -1, 0), (-1, 1, 0), (-1, -1, 0), (1, 0, 1), (1, 0, -1), (-1, 0, 1), (-1, 0, -1), (0, 1, 1), (0, 1, -1), (0, -1, 1), (0, -1, -1))

def neighbour_table(size_x, size_y, size_z):
    lookup = np.zeros((size_x * size_y * size_z, len(SHELL_VECTORS)), np.int32)
    for place_x in range(size_x):
        for place_y in range(size_y):
            for place_z in range(size_z):
                flat_index = (place_x * size_y + place_y) * size_z + place_z
                for column, shell in enumerate(SHELL_VECTORS):
                    target_x = (place_x + shell[0]) % size_x
                    target_y = (place_y + shell[1]) % size_y
                    target_z = (place_z + shell[2]) % size_z
                    lookup[flat_index, column] = (target_x * size_y + target_y) * size_z + target_z
    return lookup

def stack_complex(matrix, half_cols):
    real_part = matrix[..., :half_cols]
    imag_part = matrix[..., half_cols:]
    upper_half = jnp.concatenate([real_part, imag_part], axis=-1)
    lower_half = jnp.concatenate([-imag_part, real_part], axis=-1)
    return jnp.concatenate([upper_half, lower_half], axis=-2)

def gram_parts(iterate, half_cols):
    blocks = jnp.dot(iterate.T, iterate, precision=lax.Precision.HIGHEST)
    real_part = blocks[:half_cols, :half_cols] + blocks[half_cols:, half_cols:]
    imag_part = blocks[:half_cols, half_cols:] - blocks[half_cols:, :half_cols]
    return jnp.concatenate([real_part, imag_part], axis=1)

def sweep_step(iterate, gram_sum, half_cols):
    identity = jnp.eye(half_cols, dtype=jnp.float32)
    factor = jnp.concatenate([1.5 * identity - 0.5 * gram_sum[:, :half_cols], -0.5 * gram_sum[:, half_cols:]], axis=1)
    return jnp.dot(iterate, stack_complex(factor, half_cols), precision=lax.Precision.HIGHEST)

def assemble(mine, whole, weights, half_cols):
    real_part = mine[..., :half_cols]
    imag_part = mine[..., half_cols:]
    left_rows = jnp.concatenate([mine, jnp.concatenate([imag_part, -real_part], axis=-1)], axis=-2)
    products = jnp.einsum('brc,bsc->brs', left_rows.astype(jnp.float32), whole.astype(jnp.float32), precision=lax.Precision.HIGHEST)
    summed = jnp.einsum('b,brs->rs', weights, products, precision=lax.Precision.HIGHEST)
    row_count = mine.shape[-2]
    return jnp.concatenate([summed[:row_count], summed[row_count:]], axis=1)

def reference(margins, subspace, shell_weights, window_count):
    lookup = jnp.asarray(neighbour_table(KX, KY, KZ)).astype(jnp.int32)
    row_index = lax.iota(jnp.int32, NB)

    def one_point(payload):
        margin, window, targets, current = payload
        nearby = jnp.take(subspace, targets, axis=0)
        products = jnp.einsum('brc,bcs->brs', margin.astype(jnp.float32), stack_complex(nearby, NW).astype(jnp.float32), precision=lax.Precision.HIGHEST)
        projected = jnp.where((row_index < window)[None, :, None], products, 0.0).astype(jnp.bfloat16)
        assembled = assemble(projected, projected, shell_weights, NW)
        iterate = jnp.dot(assembled, stack_complex(current.astype(jnp.float32), NW), precision=lax.Precision.HIGHEST)
        squares = jnp.sum(iterate * iterate)
        iterate = iterate * lax.rsqrt(2.0 * squares / NW + 1e-06)
        for sweep_number in range(SWEEPS):
            iterate = sweep_step(iterate, gram_parts(iterate, NW), NW)
        return iterate * math.sqrt(NB)
    return lax.map(one_point, (margins, window_count, lookup, subspace))
```

```python
import functools
import math

import jax
import jax.numpy as jnp
from jax import lax
from jax.experimental import pallas as pl
from jax.experimental.pallas import tpu as pltpu
from jax.sharding import PartitionSpec as P

SHELL_VECTORS = (
    (1, 1, 0),
    (1, -1, 0),
    (-1, 1, 0),
    (-1, -1, 0),
    (1, 0, 1),
    (1, 0, -1),
    (-1, 0, 1),
    (-1, 0, -1),
    (0, 1, 1),
    (0, 1, -1),
    (0, -1, 1),
    (0, -1, -1),
)
BATCH = 4
VMEM = pl.BlockSpec(memory_space=pltpu.VMEM)
SMEM = pl.BlockSpec(memory_space=pltpu.SMEM)
F32 = jnp.float32
BF16 = jnp.bfloat16
NT = (((1,), (1,)), ((), ()))
TN = (((0,), (0,)), ((), ()))


def grid_shape(point_count):
    size_y = min(4, point_count // 8)
    return (4, size_y, point_count // (4 * size_y))


def displacement(shell, point_count):
    return tuple(step % size for step, size in zip(shell, grid_shape(point_count)))


def fetch_pairs(shift, point_count):
    size_x, size_y, size_z = grid_shape(point_count)
    pairs = []
    for x in range(size_x):
        for y in range(size_y):
            for z in range(size_z):
                source = ((x + shift[0]) % size_x, (y + shift[1]) % size_y, (z + shift[2]) % size_z)
                pairs.append(
                    (
                        (source[0] * size_y + source[1]) * size_z + source[2],
                        (x * size_y + y) * size_z + z,
                    )
                )
    return pairs


def dot(left, right, dims=None):
    if dims is None:
        return jnp.dot(left, right, preferred_element_type=F32)
    return lax.dot_general(left, right, dims, preferred_element_type=F32)


def split(value):
    high = value.astype(BF16)
    return high, (value - high.astype(F32)).astype(BF16)


def dot_exact_right(left, right, dims=None):
    high, low = split(left)
    return dot(high, right, dims) + dot(low, right, dims)


def dot_split(left, right, dims=None):
    left_high, left_low = split(left)
    right_high, right_low = split(right)
    return (
        dot(left_high, right_high, dims)
        + dot(left_high, right_low, dims)
        + dot(left_low, right_high, dims)
    )


def times_minus_i(value):
    half = value.shape[-1] // 2
    return jnp.concatenate([value[:, half:], -value[:, :half]], axis=1)


def times_i(value):
    half = value.shape[-1] // 2
    return jnp.concatenate([-value[:, half:], value[:, :half]], axis=1)


def stack_halves(mine, other, side, rows_ref):
    rows = mine.shape[0]
    rows_ref[pl.ds(pl.multiple_of(side * rows, 8), rows), :] = mine[...].astype(F32)
    rows_ref[pl.ds(pl.multiple_of((1 - side) * rows, 8), rows), :] = other[...].astype(F32)


def project_kernel(
    groups, first, has_total, place_ref, root_ref, margins_ref, *refs
):
    halves = refs[: 2 * len(groups)]
    refs = refs[2 * len(groups) :]
    if has_total:
        before_ref, *refs = refs
    keep_ref, send_ref, total_ref, rows_ref, stacked_ref, blocks_ref = refs
    side, limit = place_ref[0], place_ref[1]
    rows = margins_ref.shape[2]
    full = 2 * rows
    mask = lax.broadcasted_iota(jnp.int32, (rows, 1), 0) < limit
    real = jnp.zeros((rows, rows), F32)
    imag = jnp.zeros((rows, rows), F32)
    if has_total:
        real, imag = before_ref[0], before_ref[1]
    for number, members in enumerate(groups):
        stack_halves(halves[2 * number], halves[2 * number + 1], side, rows_ref)
        whole = rows_ref[...]
        stacked_ref[:full, :] = whole.astype(BF16)
        stacked_ref[full:, :] = times_i(whole).astype(BF16)
        for member in members:
            product = dot(margins_ref[0, member], stacked_ref[...])
            block = jnp.where(mask, product * root_ref[first + member], 0.0).astype(BF16)
            blocks_ref[member] = block
            real += dot(block, block, NT)
            imag += dot(times_minus_i(block), block, NT)
    for pair in range(BATCH // 2):
        keep_ref[pair] = blocks_ref[2 * pair + side]
        send_ref[pair] = blocks_ref[2 * pair + 1 - side]
    total_ref[0] = real
    total_ref[1] = imag


def project(place, roots, margins, batch, groups, halves, before):
    rows, double = margins.shape[2:]
    width = halves[0].shape[-1]
    pairs = BATCH // 2
    has_total = before is not None
    operands = [place, roots, margins, *halves] + ([before] if has_total else [])
    in_specs = [
        SMEM,
        SMEM,
        pl.BlockSpec((1, BATCH, rows, double), lambda step: (0, batch, 0, 0)),
        *([VMEM] * (len(operands) - 3)),
    ]
    block = jax.ShapeDtypeStruct((pairs, rows, width), BF16)
    return pl.pallas_call(
        functools.partial(project_kernel, groups, batch * BATCH, has_total),
        grid=(1,),
        in_specs=in_specs,
        out_specs=[VMEM] * 3,
        out_shape=[block, block, jax.ShapeDtypeStruct((2, rows, rows), F32)],
        scratch_shapes=[
            pltpu.VMEM((2 * rows, width), F32),
            pltpu.VMEM((2 * double // 2, width), BF16),
            pltpu.VMEM((BATCH, rows, width), BF16),
        ],
        cost_estimate=pl.CostEstimate(
            flops=2 * BATCH * rows * double * width * 2,
            bytes_accessed=2 * BATCH * rows * double,
            transcendentals=0,
        ),
        name=f"project_{batch}",
    )(*operands)


def cross_kernel(count, final, *refs):
    keeps, gots = refs[:count], refs[count : 2 * count]
    mine_ref, theirs_ref = refs[2 * count :]
    rows = keeps[0].shape[1]
    sums = [jnp.zeros((rows, rows), F32) for _ in range(4)]
    for keep_ref, got_ref in zip(keeps, gots):
        for pair in range(keep_ref.shape[0]):
            keep, got = keep_ref[pair], got_ref[pair]
            sums[0] += dot(keep, got, NT)
            sums[1] += dot(times_minus_i(keep), got, NT)
            sums[2] += dot(got, keep, NT)
            sums[3] += dot(times_minus_i(got), keep, NT)
    mine_ref[0], mine_ref[1] = sums[0], sums[1]
    theirs_ref[0], theirs_ref[1] = sums[2].astype(BF16), sums[3].astype(BF16)


def cross(keeps, gots):
    pairs, rows, width = keeps[0].shape
    count = len(keeps)
    return pl.pallas_call(
        functools.partial(cross_kernel, count, True),
        in_specs=[VMEM] * (2 * count),
        out_specs=[VMEM] * 2,
        out_shape=[
            jax.ShapeDtypeStruct((2, rows, rows), F32),
            jax.ShapeDtypeStruct((2, rows, rows), BF16),
        ],
        cost_estimate=pl.CostEstimate(
            flops=8 * 2 * count * pairs * rows * rows * width,
            bytes_accessed=4 * count * pairs * rows * width,
            transcendentals=0,
        ),
        name="cross",
    )(*keeps, *gots)


def complex_stack(value):
    return jnp.concatenate([value, times_i(value)], axis=0)


def update_kernel(
    scale, own_ref, other_ref, own_total_ref, other_total_ref, mine_ref, theirs_ref, out_ref
):
    own, other = own_ref[...], other_ref[...]
    half = own.shape[1] // 2
    own_i, other_i = times_i(own.astype(F32)).astype(BF16), times_i(other.astype(F32)).astype(BF16)
    cross_real = mine_ref[0] + theirs_ref[0].astype(F32)
    cross_imag = mine_ref[1] + theirs_ref[1].astype(F32)
    product = (
        dot_exact_right(own_total_ref[0], own)
        + dot_exact_right(own_total_ref[1], own_i)
        + dot_exact_right(cross_real, other)
        + dot_exact_right(cross_imag, other_i)
    )
    product_other = (
        dot(other_total_ref[0], other)
        + dot(other_total_ref[1], other_i)
        + dot_exact_right(cross_real, own, TN)
        - dot_exact_right(cross_imag, own_i, TN)
    )
    blocks = dot_split(product, product, TN) + dot_split(product_other, product_other, TN)
    real = blocks[:half, :half] + blocks[half:, half:]
    imag = blocks[:half, half:] - blocks[half:, :half]
    diagonal = lax.broadcasted_iota(jnp.int32, (half, 2 * half), 0) == lax.broadcasted_iota(
        jnp.int32, (half, 2 * half), 1
    )
    gram = jnp.concatenate([real, imag], axis=1)
    squares = jnp.sum(jnp.where(diagonal, gram, 0.0))
    size = jnp.full((1, 1), 2.0 * squares / half + 1e-06, F32)
    scaling = lax.rsqrt(size)
    gram = gram * (scaling * scaling)
    identity = jnp.where(diagonal, 1.0, 0.0)
    gram_two = dot_split(gram, complex_stack(gram))
    left = 2.25 * identity - 1.5 * gram + 0.25 * gram_two
    right = 1.5 * gram - 0.5 * gram_two
    factor = 2.25 * identity - 0.75 * gram - 0.5 * dot_split(left, complex_stack(right))
    factor = factor * (scaling * scale)
    out_ref[0] = dot_split(product, complex_stack(factor))


def update(scale, own, other, own_total, other_total, mine, theirs):
    rows, width = own.shape
    return pl.pallas_call(
        functools.partial(update_kernel, scale),
        in_specs=[VMEM] * 6,
        out_specs=VMEM,
        out_shape=jax.ShapeDtypeStruct((1, rows, width), F32),
        name="update",
    )(own, other, own_total, other_total, mine, theirs)


def on_device(margins, subspace, shell_weights, window_count):
    point_count = lax.axis_size("kpt")
    side = lax.axis_index("band")
    rows = subspace.shape[1]
    own = subspace[0]
    swap = [(0, 1), (1, 0)]
    place = jnp.stack([side, window_count[0] - side * rows])
    roots = jnp.sqrt(shell_weights)
    other = lax.ppermute(own, "band", swap)
    total = None
    keeps, gots = [], []
    plan = []
    for batch in reversed(range(len(SHELL_VECTORS) // BATCH)):
        shifts = {}
        for member in range(BATCH):
            shift = displacement(SHELL_VECTORS[batch * BATCH + member], point_count)
            shifts.setdefault(shift, []).append(member)
        plan.append((batch, shifts))
    fetched = [
        [lax.ppermute(own, "kpt", fetch_pairs(shift, point_count)) for shift in shifts]
        for _, shifts in plan
    ]
    for (batch, shifts), firsts in zip(plan, fetched):
        halves = []
        for shift, first in zip(shifts, firsts):
            halves += [first, lax.ppermute(other, "kpt", fetch_pairs(shift, point_count))]
        keep, send, total = project(
            place, roots, margins, batch, list(shifts.values()), halves, total
        )
        keeps.append(keep)
        gots.append(lax.ppermute(send, "band", swap))
    other_total = lax.ppermute(total.astype(BF16), "band", swap)
    mine, theirs = cross(keeps, gots)
    theirs = lax.ppermute(theirs, "band", swap)
    scale = math.sqrt(rows * lax.axis_size("band"))
    return update(scale, own, other, total, other_total, mine, theirs)


def solution(mesh):
    return jax.shard_map(
        on_device,
        mesh=mesh,
        in_specs=(P("kpt", None, "band", None), P("kpt", "band", None), P(), P("kpt")),
        out_specs=P("kpt", "band", None),
        check_vma=False,
    )
```

```python
import functools
import math

import jax
import jax.numpy as jnp
from jax import lax
from jax.experimental import pallas as pl
from jax.experimental.pallas import tpu as pltpu
from jax.sharding import PartitionSpec as P


SHELL_VECTORS = (
    (1, 1, 0),
    (1, -1, 0),
    (-1, 1, 0),
    (-1, -1, 0),
    (1, 0, 1),
    (1, 0, -1),
    (-1, 0, 1),
    (-1, 0, -1),
    (0, 1, 1),
    (0, 1, -1),
    (0, -1, 1),
    (0, -1, -1),
)
BATCH = 4
VMEM = pl.BlockSpec(memory_space=pltpu.VMEM)
SMEM = pl.BlockSpec(memory_space=pltpu.SMEM)
F32 = jnp.float32
BF16 = jnp.bfloat16
NT = (((1,), (1,)), ((), ()))
TN = (((0,), (0,)), ((), ()))


def grid_shape(point_count):
    size_y = min(4, point_count // 8)
    return (4, size_y, point_count // (4 * size_y))


def displacement(shell, point_count):
    return tuple(step % size for step, size in zip(shell, grid_shape(point_count)))


def fetch_pairs(shift, point_count):
    size_x, size_y, size_z = grid_shape(point_count)
    pairs = []
    for x in range(size_x):
        for y in range(size_y):
            for z in range(size_z):
                source = ((x + shift[0]) % size_x, (y + shift[1]) % size_y, (z + shift[2]) % size_z)
                pairs.append(
                    (
                        (source[0] * size_y + source[1]) * size_z + source[2],
                        (x * size_y + y) * size_z + z,
                    )
                )
    return pairs


def dot(left, right, dims=None):
    if dims is None:
        return jnp.dot(left, right, preferred_element_type=F32)
    return lax.dot_general(left, right, dims, preferred_element_type=F32)


def split(value):
    high = value.astype(BF16)
    return high, (value - high.astype(F32)).astype(BF16)


def dot_exact_right(left, right, dims=None):
    high, low = split(left)
    return dot(high, right, dims) + dot(low, right, dims)


def dot_split(left, right, dims=None):
    left_high, left_low = split(left)
    right_high, right_low = split(right)
    return (
        dot(left_high, right_high, dims)
        + dot(left_high, right_low, dims)
        + dot(left_low, right_high, dims)
    )


def times_minus_i(value):
    half = value.shape[-1] // 2
    return jnp.concatenate([value[:, half:], -value[:, :half]], axis=1)


def times_i(value):
    half = value.shape[-1] // 2
    return jnp.concatenate([-value[:, half:], value[:, :half]], axis=1)


def stack_halves(mine, other, side, rows_ref):
    rows = mine.shape[0]
    rows_ref[pl.ds(pl.multiple_of(side * rows, 8), rows), :] = mine[...].astype(F32)
    rows_ref[pl.ds(pl.multiple_of((1 - side) * rows, 8), rows), :] = other[...].astype(F32)


def project_kernel(groups, first, place_ref, root_ref, margins_ref, *refs):
    halves = refs[: 2 * len(groups)]
    keep_ref, send_ref, rows_ref, stacked_ref, blocks_ref = refs[2 * len(groups) :]
    side, limit = place_ref[0], place_ref[1]
    rows = margins_ref.shape[2]
    full = 2 * rows
    mask = lax.broadcasted_iota(jnp.int32, (rows, 1), 0) < limit
    for number, members in enumerate(groups):
        stack_halves(halves[2 * number], halves[2 * number + 1], side, rows_ref)
        whole = rows_ref[...]
        stacked_ref[:full, :] = whole.astype(BF16)
        stacked_ref[full:, :] = times_i(whole).astype(BF16)
        for member in members:
            product = dot(margins_ref[0, member], stacked_ref[...])
            block = jnp.where(mask, product * root_ref[first + member], 0.0)
            blocks_ref[member] = block.astype(BF16)
    for pair in range(BATCH // 2):
        keep_ref[pair] = blocks_ref[2 * pair + side]
        send_ref[pair] = blocks_ref[2 * pair + 1 - side]


def project(place, roots, margins, batch, groups, halves):
    rows, double = margins.shape[2:]
    width = halves[0].shape[-1]
    pairs = BATCH // 2
    block = jax.ShapeDtypeStruct((pairs, rows, width), BF16)
    return pl.pallas_call(
        functools.partial(project_kernel, groups, batch * BATCH),
        grid=(1,),
        in_specs=[
            SMEM,
            SMEM,
            pl.BlockSpec((1, BATCH, rows, double), lambda step: (0, batch, 0, 0)),
            *([VMEM] * len(halves)),
        ],
        out_specs=[VMEM] * 2,
        out_shape=[block, block],
        scratch_shapes=[
            pltpu.VMEM((2 * rows, width), F32),
            pltpu.VMEM((double, width), BF16),
            pltpu.VMEM((BATCH, rows, width), BF16),
        ],
        cost_estimate=pl.CostEstimate(
            flops=2 * BATCH * rows * double * width,
            bytes_accessed=2 * BATCH * rows * double,
            transcendentals=0,
        ),
    )(place, roots, margins, *halves)


def gather_own_kernel(count, has_total, *refs):
    blocks, refs = refs[:count], refs[count:]
    rows = blocks[0].shape[1]
    real = jnp.zeros((rows, rows), F32)
    imag = jnp.zeros((rows, rows), F32)
    if has_total:
        real, imag = refs[0][0], refs[0][1]
    for block_ref in blocks:
        for pair in range(block_ref.shape[0]):
            block = block_ref[pair]
            real += dot(block, block, NT)
            imag += dot(times_minus_i(block), block, NT)
    for total_ref in refs[1 if has_total else 0 :]:
        total_ref[0] = real.astype(total_ref.dtype)
        total_ref[1] = imag.astype(total_ref.dtype)


def gather_own(blocks, before):
    pairs, rows, width = blocks[0].shape
    count = len(blocks)
    operands = list(blocks) + ([] if before is None else [before])
    kinds = [F32] if before is None else [F32, BF16]
    return pl.pallas_call(
        functools.partial(gather_own_kernel, count, before is not None),
        in_specs=[VMEM] * len(operands),
        out_specs=[VMEM] * len(kinds),
        out_shape=[jax.ShapeDtypeStruct((2, rows, rows), kind) for kind in kinds],
        cost_estimate=pl.CostEstimate(
            flops=4 * count * pairs * rows * rows * width,
            bytes_accessed=2 * count * pairs * rows * width,
            transcendentals=0,
        ),
    )(*operands)


def cross_kernel(has_total, keep_ref, got_ref, *refs):
    if has_total:
        mine_before_ref, theirs_before_ref, *refs = refs
    mine_ref, theirs_ref = refs
    rows = keep_ref.shape[1]
    sums = [jnp.zeros((rows, rows), F32) for _ in range(4)]
    if has_total:
        sums = [mine_before_ref[0], mine_before_ref[1], theirs_before_ref[0], theirs_before_ref[1]]
    for pair in range(keep_ref.shape[0]):
        keep, got = keep_ref[pair], got_ref[pair]
        sums[0] += dot(keep, got, NT)
        sums[1] += dot(times_minus_i(keep), got, NT)
        sums[2] += dot(got, keep, NT)
        sums[3] += dot(times_minus_i(got), keep, NT)
    mine_ref[0], mine_ref[1] = sums[0], sums[1]
    kind = theirs_ref.dtype
    theirs_ref[0], theirs_ref[1] = sums[2].astype(kind), sums[3].astype(kind)


def cross(keep, got, before, last):
    pairs, rows, width = keep.shape
    operands = [keep, got, *(before or ())]
    return pl.pallas_call(
        functools.partial(cross_kernel, before is not None),
        in_specs=[VMEM] * len(operands),
        out_specs=[VMEM] * 2,
        out_shape=[
            jax.ShapeDtypeStruct((2, rows, rows), F32),
            jax.ShapeDtypeStruct((2, rows, rows), BF16 if last else F32),
        ],
        cost_estimate=pl.CostEstimate(
            flops=8 * 2 * pairs * rows * rows * width,
            bytes_accessed=4 * pairs * rows * width,
            transcendentals=0,
        ),
    )(*operands)


def complex_stack(value):
    return jnp.concatenate([value, times_i(value)], axis=0)


def update_kernel(
    scale, own_ref, other_ref, own_total_ref, other_total_ref, mine_ref, theirs_ref, out_ref
):
    own, other = own_ref[...], other_ref[...]
    half = own.shape[1] // 2
    own_i, other_i = times_i(own.astype(F32)).astype(BF16), times_i(other.astype(F32)).astype(BF16)
    cross_real = mine_ref[0] + theirs_ref[0].astype(F32)
    cross_imag = mine_ref[1] + theirs_ref[1].astype(F32)
    product = (
        dot_exact_right(own_total_ref[0], own)
        + dot_exact_right(own_total_ref[1], own_i)
        + dot_exact_right(cross_real, other)
        + dot_exact_right(cross_imag, other_i)
    )
    product_other = (
        dot(other_total_ref[0], other)
        + dot(other_total_ref[1], other_i)
        + dot_exact_right(cross_real, own, TN)
        - dot_exact_right(cross_imag, own_i, TN)
    )
    blocks = dot_split(product, product, TN) + dot_split(product_other, product_other, TN)
    real = blocks[:half, :half] + blocks[half:, half:]
    imag = blocks[:half, half:] - blocks[half:, :half]
    diagonal = lax.broadcasted_iota(jnp.int32, (half, 2 * half), 0) == lax.broadcasted_iota(
        jnp.int32, (half, 2 * half), 1
    )
    gram = jnp.concatenate([real, imag], axis=1)
    squares = jnp.sum(jnp.where(diagonal, gram, 0.0))
    size = jnp.full((1, 1), 2.0 * squares / half + 1e-06, F32)
    scaling = lax.rsqrt(size)
    gram = gram * (scaling * scaling)
    identity = jnp.where(diagonal, 1.0, 0.0)
    gram_two = dot_split(gram, complex_stack(gram))
    left = 2.25 * identity - 1.5 * gram + 0.25 * gram_two
    right = 1.5 * gram - 0.5 * gram_two
    factor = 2.25 * identity - 0.75 * gram - 0.5 * dot_split(left, complex_stack(right))
    factor = factor * (scaling * scale)
    out_ref[0] = dot_split(product, complex_stack(factor))


def update(scale, own, other, own_total, other_total, mine, theirs):
    rows, width = own.shape
    return pl.pallas_call(
        functools.partial(update_kernel, scale),
        in_specs=[VMEM] * 6,
        out_specs=VMEM,
        out_shape=jax.ShapeDtypeStruct((1, rows, width), F32),
        name="update",
    )(own, other, own_total, other_total, mine, theirs)


def batch_shifts(batch, point_count):
    shifts = {}
    for member in range(BATCH):
        shift = displacement(SHELL_VECTORS[batch * BATCH + member], point_count)
        shifts.setdefault(shift, []).append(member)
    return shifts


def on_device(margins, subspace, shell_weights, window_count):
    point_count = lax.axis_size("kpt")
    side = lax.axis_index("band")
    rows = subspace.shape[1]
    swap = [(0, 1), (1, 0)]
    plan = [batch_shifts(batch, point_count) for batch in range(3)]

    def exchange(value):
        return lax.ppermute(value, "band", swap)

    def fetch(value, shift):
        return lax.ppermute(value, "kpt", fetch_pairs(shift, point_count))

    place = jnp.stack([side, window_count[0] - side * rows])
    roots = jnp.sqrt(shell_weights)
    own = subspace[0]
    other = exchange(own)
    halves = {}
    for part, value in (("own", own), ("other", other)):
        for batch in (2, 1):
            for shift in plan[batch]:
                halves[batch, part, shift] = fetch(value, shift)
        for shift in plan[0]:
            near = displacement((shift[0], 0, 1), point_count)
            step = displacement((0, shift[1], -1), point_count)
            halves[0, part, shift] = fetch(halves[1, part, near], step)
    kept, given, got = {}, {}, {}
    total, crossed = None, None
    for batch in (2, 1, 0):
        blocks = []
        for shift in plan[batch]:
            blocks += [halves[batch, "own", shift], halves[batch, "other", shift]]
        kept[batch], given[batch] = project(
            place, roots, margins, batch, list(plan[batch].values()), blocks
        )
        got[batch] = exchange(given[batch])
    (total,) = gather_own([kept[2], given[2], kept[1], given[1]], None)
    total, total_sent = gather_own([kept[0], given[0]], total)
    other_total = exchange(total_sent)
    for batch in (2, 1, 0):
        crossed = cross(kept[batch], got[batch], crossed, batch == 0)
    mine, theirs = crossed
    theirs = exchange(theirs)
    scale = math.sqrt(rows * lax.axis_size("band"))
    return update(scale, own, other, total, other_total, mine, theirs)


def solution(mesh):
    return jax.shard_map(
        on_device,
        mesh=mesh,
        in_specs=(P("kpt", None, "band", None), P("kpt", "band", None), P(), P("kpt")),
        out_specs=P("kpt", "band", None),
        check_vma=False,
    )
```

```python
import functools
import math

import jax
import jax.numpy as jnp
from jax import lax
from jax.experimental import pallas as pl
from jax.experimental.pallas import tpu as pltpu
from jax.sharding import PartitionSpec as P


SHELL_VECTORS = (
    (1, 1, 0),
    (1, -1, 0),
    (-1, 1, 0),
    (-1, -1, 0),
    (1, 0, 1),
    (1, 0, -1),
    (-1, 0, 1),
    (-1, 0, -1),
    (0, 1, 1),
    (0, 1, -1),
    (0, -1, 1),
    (0, -1, -1),
)
BATCH = 4
VMEM = pl.BlockSpec(memory_space=pltpu.VMEM)
LIMIT = pltpu.CompilerParams(vmem_limit_bytes=20 * 2**20)
SMEM = pl.BlockSpec(memory_space=pltpu.SMEM)
F32 = jnp.float32
BF16 = jnp.bfloat16
NT = (((1,), (1,)), ((), ()))
TN = (((0,), (0,)), ((), ()))


def grid_shape(point_count):
    size_y = min(4, point_count // 8)
    return (4, size_y, point_count // (4 * size_y))


def displacement(shell, point_count):
    return tuple(step % size for step, size in zip(shell, grid_shape(point_count)))


def fetch_pairs(shift, point_count):
    size_x, size_y, size_z = grid_shape(point_count)
    pairs = []
    for x in range(size_x):
        for y in range(size_y):
            for z in range(size_z):
                source = ((x + shift[0]) % size_x, (y + shift[1]) % size_y, (z + shift[2]) % size_z)
                pairs.append(
                    (
                        (source[0] * size_y + source[1]) * size_z + source[2],
                        (x * size_y + y) * size_z + z,
                    )
                )
    return pairs


def dot(left, right, dims=None):
    if dims is None:
        return jnp.dot(left, right, preferred_element_type=F32)
    return lax.dot_general(left, right, dims, preferred_element_type=F32)


def split(value):
    high = value.astype(BF16)
    return high, (value - high.astype(F32)).astype(BF16)


def dot_exact_right(left, right, dims=None):
    high, low = split(left)
    return dot(high, right, dims) + dot(low, right, dims)


def dot_split(left, right, dims=None):
    left_high, left_low = split(left)
    right_high, right_low = split(right)
    return (
        dot(left_high, right_high, dims)
        + dot(left_high, right_low, dims)
        + dot(left_low, right_high, dims)
    )


def times_minus_i(value):
    half = value.shape[-1] // 2
    return jnp.concatenate([value[:, half:], -value[:, :half]], axis=1)


def times_i(value):
    half = value.shape[-1] // 2
    return jnp.concatenate([-value[:, half:], value[:, :half]], axis=1)


def stack_halves(mine, other, side, rows_ref):
    rows = mine.shape[0]
    rows_ref[pl.ds(pl.multiple_of(side * rows, 8), rows), :] = mine[...].astype(F32)
    rows_ref[pl.ds(pl.multiple_of((1 - side) * rows, 8), rows), :] = other[...].astype(F32)


def project_kernel(groups, first, place_ref, root_ref, margins_ref, *refs):
    halves = refs[: 2 * len(groups)]
    keep_ref, send_ref, rows_ref, stacked_ref, blocks_ref = refs[2 * len(groups) :]
    side, limit = place_ref[0], place_ref[1]
    rows = margins_ref.shape[2]
    full = 2 * rows
    mask = lax.broadcasted_iota(jnp.int32, (rows, 1), 0) < limit
    for number, members in enumerate(groups):
        stack_halves(halves[2 * number], halves[2 * number + 1], side, rows_ref)
        whole = rows_ref[...]
        stacked_ref[:full, :] = whole.astype(BF16)
        stacked_ref[full:, :] = times_i(whole).astype(BF16)
        for member in members:
            product = dot(margins_ref[0, first + member], stacked_ref[...])
            block = jnp.where(mask, product * root_ref[first + member], 0.0)
            blocks_ref[member] = block.astype(BF16)
    for pair in range(BATCH // 2):
        keep_ref[pair] = blocks_ref[2 * pair + side]
        send_ref[pair] = blocks_ref[2 * pair + 1 - side]


def project(place, roots, margins, batch, groups, halves):
    rows, double = margins.shape[2:]
    width = halves[0].shape[-1]
    pairs = BATCH // 2
    block = jax.ShapeDtypeStruct((pairs, rows, width), BF16)
    return pl.pallas_call(
        functools.partial(project_kernel, groups, batch * BATCH),
        in_specs=[SMEM, SMEM, VMEM, *([VMEM] * len(halves))],
        out_specs=[VMEM] * 2,
        out_shape=[block, block],
        scratch_shapes=[
            pltpu.VMEM((2 * rows, width), F32),
            pltpu.VMEM((double, width), BF16),
            pltpu.VMEM((BATCH, rows, width), BF16),
        ],
        cost_estimate=pl.CostEstimate(
            flops=2 * BATCH * rows * double * width,
            bytes_accessed=2 * BATCH * rows * double,
            transcendentals=0,
        ),
        compiler_params=LIMIT,
    )(place, roots, margins, *halves)


def gather_own_kernel(count, has_total, *refs):
    blocks, refs = refs[:count], refs[count:]
    rows = blocks[0].shape[1]
    real = jnp.zeros((rows, rows), F32)
    imag = jnp.zeros((rows, rows), F32)
    if has_total:
        real, imag = refs[0][0], refs[0][1]
    for block_ref in blocks:
        for pair in range(block_ref.shape[0]):
            block = block_ref[pair]
            real += dot(block, block, NT)
            imag += dot(times_minus_i(block), block, NT)
    for total_ref in refs[1 if has_total else 0 :]:
        total_ref[0] = real.astype(total_ref.dtype)
        total_ref[1] = imag.astype(total_ref.dtype)


def gather_own(blocks, before):
    pairs, rows, width = blocks[0].shape
    count = len(blocks)
    operands = list(blocks) + ([] if before is None else [before])
    kinds = [F32] if before is None else [F32, BF16]
    return pl.pallas_call(
        functools.partial(gather_own_kernel, count, before is not None),
        in_specs=[VMEM] * len(operands),
        out_specs=[VMEM] * len(kinds),
        out_shape=[jax.ShapeDtypeStruct((2, rows, rows), kind) for kind in kinds],
        cost_estimate=pl.CostEstimate(
            flops=4 * count * pairs * rows * rows * width,
            bytes_accessed=2 * count * pairs * rows * width,
            transcendentals=0,
        ),
        compiler_params=LIMIT,
    )(*operands)


def cross_kernel(has_total, keep_ref, got_ref, *refs):
    if has_total:
        mine_before_ref, theirs_before_ref, *refs = refs
    mine_ref, theirs_ref = refs
    rows = keep_ref.shape[1]
    sums = [jnp.zeros((rows, rows), F32) for _ in range(4)]
    if has_total:
        sums = [mine_before_ref[0], mine_before_ref[1], theirs_before_ref[0], theirs_before_ref[1]]
    for pair in range(keep_ref.shape[0]):
        keep, got = keep_ref[pair], got_ref[pair]
        sums[0] += dot(keep, got, NT)
        sums[1] += dot(times_minus_i(keep), got, NT)
        sums[2] += dot(got, keep, NT)
        sums[3] += dot(times_minus_i(got), keep, NT)
    mine_ref[0], mine_ref[1] = sums[0], sums[1]
    kind = theirs_ref.dtype
    theirs_ref[0], theirs_ref[1] = sums[2].astype(kind), sums[3].astype(kind)


def cross(keep, got, before, last):
    pairs, rows, width = keep.shape
    operands = [keep, got, *(before or ())]
    return pl.pallas_call(
        functools.partial(cross_kernel, before is not None),
        in_specs=[VMEM] * len(operands),
        out_specs=[VMEM] * 2,
        out_shape=[
            jax.ShapeDtypeStruct((2, rows, rows), F32),
            jax.ShapeDtypeStruct((2, rows, rows), BF16 if last else F32),
        ],
        cost_estimate=pl.CostEstimate(
            flops=8 * 2 * pairs * rows * rows * width,
            bytes_accessed=4 * pairs * rows * width,
            transcendentals=0,
        ),
        compiler_params=LIMIT,
    )(*operands)


def complex_stack(value):
    return jnp.concatenate([value, times_i(value)], axis=0)


def update_kernel(
    scale, own_ref, other_ref, own_total_ref, other_total_ref, mine_ref, theirs_ref, out_ref
):
    own, other = own_ref[...], other_ref[...]
    half = own.shape[1] // 2
    own_i, other_i = times_i(own.astype(F32)).astype(BF16), times_i(other.astype(F32)).astype(BF16)
    cross_real = mine_ref[0] + theirs_ref[0].astype(F32)
    cross_imag = mine_ref[1] + theirs_ref[1].astype(F32)
    product = (
        dot_exact_right(own_total_ref[0], own)
        + dot_exact_right(own_total_ref[1], own_i)
        + dot_exact_right(cross_real, other)
        + dot_exact_right(cross_imag, other_i)
    )
    product_other = (
        dot(other_total_ref[0], other)
        + dot(other_total_ref[1], other_i)
        + dot_exact_right(cross_real, own, TN)
        - dot_exact_right(cross_imag, own_i, TN)
    )
    blocks = dot_split(product, product, TN) + dot_split(product_other, product_other, TN)
    real = blocks[:half, :half] + blocks[half:, half:]
    imag = blocks[:half, half:] - blocks[half:, :half]
    diagonal = lax.broadcasted_iota(jnp.int32, (half, 2 * half), 0) == lax.broadcasted_iota(
        jnp.int32, (half, 2 * half), 1
    )
    gram = jnp.concatenate([real, imag], axis=1)
    squares = jnp.sum(jnp.where(diagonal, gram, 0.0))
    size = jnp.full((1, 1), 2.0 * squares / half + 1e-06, F32)
    scaling = lax.rsqrt(size)
    gram = gram * (scaling * scaling)
    identity = jnp.where(diagonal, 1.0, 0.0)
    gram_two = dot_split(gram, complex_stack(gram))
    left = 2.25 * identity - 1.5 * gram + 0.25 * gram_two
    right = 1.5 * gram - 0.5 * gram_two
    factor = 2.25 * identity - 0.75 * gram - 0.5 * dot_split(left, complex_stack(right))
    factor = factor * (scaling * scale)
    out_ref[0] = dot_split(product, complex_stack(factor))


def update(scale, own, other, own_total, other_total, mine, theirs):
    rows, width = own.shape
    return pl.pallas_call(
        functools.partial(update_kernel, scale),
        in_specs=[VMEM] * 6,
        out_specs=VMEM,
        out_shape=jax.ShapeDtypeStruct((1, rows, width), F32),
        name="update",
        compiler_params=LIMIT,
    )(own, other, own_total, other_total, mine, theirs)


def batch_shifts(batch, point_count):
    shifts = {}
    for member in range(BATCH):
        shift = displacement(SHELL_VECTORS[batch * BATCH + member], point_count)
        shifts.setdefault(shift, []).append(member)
    return shifts


def on_device(margins, subspace, shell_weights, window_count):
    point_count = lax.axis_size("kpt")
    side = lax.axis_index("band")
    rows = subspace.shape[1]
    swap = [(0, 1), (1, 0)]
    plan = [batch_shifts(batch, point_count) for batch in range(3)]

    def exchange(value):
        return lax.ppermute(value, "band", swap)

    def fetch(value, shift):
        return lax.ppermute(value, "kpt", fetch_pairs(shift, point_count))

    place = jnp.stack([side, window_count[0] - side * rows])
    roots = jnp.sqrt(shell_weights)
    own = subspace[0]
    other = exchange(own)
    halves = {}
    for part, value in (("own", own), ("other", other)):
        for batch in (2, 1):
            for shift in plan[batch]:
                halves[batch, part, shift] = fetch(value, shift)
        for shift in plan[0]:
            near = displacement((shift[0], 0, 1), point_count)
            step = displacement((0, shift[1], -1), point_count)
            halves[0, part, shift] = fetch(halves[1, part, near], step)
    kept, given, got = {}, {}, {}
    total, crossed = None, None
    for batch in (2, 1, 0):
        blocks = []
        for shift in plan[batch]:
            blocks += [halves[batch, "own", shift], halves[batch, "other", shift]]
        kept[batch], given[batch] = project(
            place, roots, margins, batch, list(plan[batch].values()), blocks
        )
        got[batch] = exchange(given[batch])
    (total,) = gather_own([kept[2], given[2], kept[1], given[1]], None)
    total, total_sent = gather_own([kept[0], given[0]], total)
    other_total = exchange(total_sent)
    for batch in (2, 1, 0):
        crossed = cross(kept[batch], got[batch], crossed, batch == 0)
    mine, theirs = crossed
    theirs = exchange(theirs)
    scale = math.sqrt(rows * lax.axis_size("band"))
    return update(scale, own, other, total, other_total, mine, theirs)


def solution(mesh):
    return jax.shard_map(
        on_device,
        mesh=mesh,
        in_specs=(P("kpt", None, "band", None), P("kpt", "band", None), P(), P("kpt")),
        out_specs=P("kpt", "band", None),
        check_vma=False,
    )
```

```python
import functools
import math

import jax
import jax.numpy as jnp
from jax import lax
from jax.experimental import pallas as pl
from jax.experimental.pallas import tpu as pltpu
from jax.sharding import PartitionSpec as P


SHELL_VECTORS = (
    (1, 1, 0),
    (1, -1, 0),
    (-1, 1, 0),
    (-1, -1, 0),
    (1, 0, 1),
    (1, 0, -1),
    (-1, 0, 1),
    (-1, 0, -1),
    (0, 1, 1),
    (0, 1, -1),
    (0, -1, 1),
    (0, -1, -1),
)
BATCH = 4
SHIPPED = 2
VMEM = pl.BlockSpec(memory_space=pltpu.VMEM)
LIMIT = pltpu.CompilerParams(vmem_limit_bytes=20 * 2**20)
SMEM = pl.BlockSpec(memory_space=pltpu.SMEM)
F32 = jnp.float32
BF16 = jnp.bfloat16
NT = (((1,), (1,)), ((), ()))
TN = (((0,), (0,)), ((), ()))


def grid_shape(point_count):
    size_y = min(4, point_count // 8)
    return (4, size_y, point_count // (4 * size_y))


def displacement(shell, point_count):
    return tuple(step % size for step, size in zip(shell, grid_shape(point_count)))


def fetch_pairs(shift, point_count):
    size_x, size_y, size_z = grid_shape(point_count)
    pairs = []
    for x in range(size_x):
        for y in range(size_y):
            for z in range(size_z):
                source = ((x + shift[0]) % size_x, (y + shift[1]) % size_y, (z + shift[2]) % size_z)
                pairs.append(
                    (
                        (source[0] * size_y + source[1]) * size_z + source[2],
                        (x * size_y + y) * size_z + z,
                    )
                )
    return pairs


def dot(left, right, dims=None):
    if dims is None:
        return jnp.dot(left, right, preferred_element_type=F32)
    return lax.dot_general(left, right, dims, preferred_element_type=F32)


def split(value):
    high = value.astype(BF16)
    return high, (value - high.astype(F32)).astype(BF16)


def dot_exact_right(left, right, dims=None):
    high, low = split(left)
    return dot(high, right, dims) + dot(low, right, dims)


def dot_split(left, right, dims=None):
    left_high, left_low = split(left)
    right_high, right_low = split(right)
    return (
        dot(left_high, right_high, dims)
        + dot(left_high, right_low, dims)
        + dot(left_low, right_high, dims)
    )


def times_minus_i(value):
    half = value.shape[-1] // 2
    return jnp.concatenate([value[:, half:], -value[:, :half]], axis=1)


def times_i(value):
    half = value.shape[-1] // 2
    return jnp.concatenate([-value[:, half:], value[:, :half]], axis=1)


def stack_complex(mine, other, side, rows_ref, stacked_ref):
    rows = mine.shape[0]
    rows_ref[pl.ds(pl.multiple_of(side * rows, 8), rows), :] = mine.astype(F32)
    rows_ref[pl.ds(pl.multiple_of((1 - side) * rows, 8), rows), :] = other.astype(F32)
    whole = rows_ref[...]
    stacked_ref[: 2 * rows, :] = whole.astype(BF16)
    stacked_ref[2 * rows :, :] = times_i(whole).astype(BF16)


def masked_block(margin, stacked, root, limit):
    inside = lax.broadcasted_iota(jnp.int32, (margin.shape[0], 1), 0) < limit
    return jnp.where(inside, dot(margin, stacked) * root, 0.0).astype(BF16)


def load_kernel(shipped, place_ref, margins_ref, all_ref, given_ref, all_sem, given_sem):
    copies = (
        pltpu.make_async_copy(margins_ref.at[0, shipped + 1 - place_ref[0]], given_ref, given_sem),
        pltpu.make_async_copy(margins_ref.at[0], all_ref, all_sem),
    )
    for copy in copies:
        copy.start()
    for copy in copies:
        copy.wait()


def load(place, margins, shipped):
    shape = margins.shape[1:]
    return pl.pallas_call(
        functools.partial(load_kernel, shipped),
        in_specs=[SMEM, pl.BlockSpec(memory_space=pl.ANY)],
        out_specs=[VMEM] * 2,
        out_shape=[
            jax.ShapeDtypeStruct(shape, margins.dtype),
            jax.ShapeDtypeStruct(shape[1:], margins.dtype),
        ],
        scratch_shapes=[pltpu.SemaphoreType.DMA] * 2,
        name="load",
        compiler_params=LIMIT,
    )(place, margins)


def project_kernel(groups, first, sent, place_ref, root_ref, margins_ref, *refs):
    halves = refs[: 2 * len(groups)]
    keep_ref, *give_refs, rows_ref, stacked_ref, blocks_ref = refs[2 * len(groups) :]
    side, limit = place_ref[0], place_ref[1]
    for number, members in enumerate(groups):
        mine, other = halves[2 * number][...], halves[2 * number + 1][...]
        stack_complex(mine, other, side, rows_ref, stacked_ref)
        for member in members:
            blocks_ref[member] = masked_block(
                margins_ref[first + member], stacked_ref[...], root_ref[first + member], limit
            )
    for pair in range(BATCH // 2):
        keep_ref[pair] = blocks_ref[2 * pair + side]
        target = give_refs[0].at[pair] if pair < sent else give_refs[1].at[pair - sent]
        target[...] = blocks_ref[2 * pair + 1 - side]


def project(place, roots, margins, batch, groups, halves, sent):
    rows, double = margins.shape[1:]
    width = halves[0].shape[-1]
    pairs = BATCH // 2
    counts = [pairs, sent] + ([pairs - sent] if sent < pairs else [])
    return pl.pallas_call(
        functools.partial(project_kernel, groups, batch * BATCH, sent),
        in_specs=[SMEM, SMEM, VMEM, *([VMEM] * len(halves))],
        out_specs=[VMEM] * len(counts),
        out_shape=[jax.ShapeDtypeStruct((count, rows, width), BF16) for count in counts],
        scratch_shapes=[
            pltpu.VMEM((2 * rows, width), F32),
            pltpu.VMEM((double, width), BF16),
            pltpu.VMEM((BATCH, rows, width), BF16),
        ],
        cost_estimate=pl.CostEstimate(
            flops=2 * BATCH * rows * double * width,
            bytes_accessed=2 * BATCH * rows * double,
            transcendentals=0,
        ),
        compiler_params=LIMIT,
    )(place, roots, margins, *halves)


def extra_kernel(shipped, place_ref, root_ref, margin_ref, *refs):
    *halves, out_ref, rows_ref, stacked_ref = refs
    side, limit = place_ref[0], place_ref[2]
    mine, other = halves[0][...], halves[1][...]
    if len(halves) > 2:
        mine = jnp.where(side == 0, mine, halves[2][...])
        other = jnp.where(side == 0, other, halves[3][...])
    stack_complex(mine, other, side, rows_ref, stacked_ref)
    root = root_ref[shipped + side]
    out_ref[0] = masked_block(margin_ref[...], stacked_ref[...], root, limit)


def extra(place, roots, margin, shipped, halves):
    rows, double = margin.shape
    width = halves[0].shape[-1]
    return pl.pallas_call(
        functools.partial(extra_kernel, shipped),
        in_specs=[SMEM, SMEM, VMEM, *([VMEM] * len(halves))],
        out_specs=VMEM,
        out_shape=jax.ShapeDtypeStruct((1, rows, width), BF16),
        scratch_shapes=[pltpu.VMEM((2 * rows, width), F32), pltpu.VMEM((double, width), BF16)],
        cost_estimate=pl.CostEstimate(
            flops=2 * rows * double * width, bytes_accessed=2 * rows * double, transcendentals=0
        ),
        name="extra",
        compiler_params=LIMIT,
    )(place, roots, margin, *halves)


def triangle(size):
    row = lax.broadcasted_iota(jnp.int32, (size, size), 0)
    return row, lax.broadcasted_iota(jnp.int32, (size, size), 1)


def gather_own_kernel(count, has_total, *refs):
    blocks, refs = refs[:count], refs[count:]
    rows = blocks[0].shape[1]
    real = jnp.zeros((rows, rows), F32)
    imag = jnp.zeros((rows, rows), F32)
    if has_total:
        real, imag = refs[0][0], refs[0][1]
    for block_ref in blocks:
        for pair in range(block_ref.shape[0]):
            block = block_ref[pair]
            real += dot(block, block, NT)
            imag += dot(times_minus_i(block), block, NT)
    total_ref, *packed = refs[1 if has_total else 0 :]
    total_ref[0], total_ref[1] = real, imag
    if packed:
        row, column = triangle(rows)
        packed[0][...] = jnp.where(row <= column, real, imag).astype(BF16)


def gather_own(blocks, before):
    rows, width = blocks[0].shape[1:]
    count = len(blocks)
    operands = list(blocks) + ([] if before is None else [before])
    results = [jax.ShapeDtypeStruct((2, rows, rows), F32)]
    if before is not None:
        results.append(jax.ShapeDtypeStruct((rows, rows), BF16))
    return pl.pallas_call(
        functools.partial(gather_own_kernel, count, before is not None),
        in_specs=[VMEM] * len(operands),
        out_specs=[VMEM] * len(results),
        out_shape=results,
        cost_estimate=pl.CostEstimate(
            flops=8 * count * rows * rows * width,
            bytes_accessed=4 * count * rows * width,
            transcendentals=0,
        ),
        compiler_params=LIMIT,
    )(*operands)


def cross_kernel(terms, count, has_total, *refs):
    blocks, refs = refs[:count], refs[count:]
    rows = blocks[0].shape[1]
    sums = [jnp.zeros((rows, rows), F32) for _ in range(4)]
    if has_total:
        mine_before_ref, theirs_before_ref, *refs = refs
        sums = [mine_before_ref[0], mine_before_ref[1], theirs_before_ref[0], theirs_before_ref[1]]
    mine_ref, theirs_ref = refs
    for keep_place, keep_index, got_place, got_index in terms:
        keep, got = blocks[keep_place][keep_index], blocks[got_place][got_index]
        sums[0] += dot(keep, got, NT)
        sums[1] += dot(times_minus_i(keep), got, NT)
        sums[2] += dot(got, keep, NT)
        sums[3] += dot(times_minus_i(got), keep, NT)
    mine_ref[0], mine_ref[1] = sums[0], sums[1]
    kind = theirs_ref.dtype
    theirs_ref[0], theirs_ref[1] = sums[2].astype(kind), sums[3].astype(kind)


def cross(blocks, terms, before, last):
    rows, width = blocks[0].shape[1:]
    operands = [*blocks, *(before or ())]
    return pl.pallas_call(
        functools.partial(cross_kernel, terms, len(blocks), before is not None),
        in_specs=[VMEM] * len(operands),
        out_specs=[VMEM] * 2,
        out_shape=[
            jax.ShapeDtypeStruct((2, rows, rows), F32),
            jax.ShapeDtypeStruct((2, rows, rows), BF16 if last else F32),
        ],
        cost_estimate=pl.CostEstimate(
            flops=8 * len(terms) * rows * rows * width,
            bytes_accessed=4 * len(terms) * rows * width,
            transcendentals=0,
        ),
        compiler_params=LIMIT,
    )(*operands)


def complex_stack(value):
    return jnp.concatenate([value, times_i(value)], axis=0)


def base_kernel(own_ref, other_ref, total_ref, packed_ref, mine_ref, base_ref, base_other_ref):
    own, other = own_ref[...], other_ref[...]
    own_i, other_i = times_i(own.astype(F32)).astype(BF16), times_i(other.astype(F32)).astype(BF16)
    real, imag = mine_ref[0], mine_ref[1]
    base_ref[...] = (
        dot_exact_right(total_ref[0], own)
        + dot_exact_right(total_ref[1], own_i)
        + dot_exact_right(real, other)
        + dot_exact_right(imag, other_i)
    )
    packed = packed_ref[...].astype(F32)
    row, column = triangle(packed.shape[0])
    upper = jnp.where(row <= column, packed, 0.0).astype(BF16)
    strict = jnp.where(row < column, packed, 0.0).astype(BF16)
    lower = jnp.where(row > column, packed, 0.0).astype(BF16)
    base_other_ref[...] = (
        dot(upper, other)
        + dot(strict, other, TN)
        + dot(lower, other_i)
        - dot(lower, other_i, TN)
        + dot_exact_right(real, own, TN)
        - dot_exact_right(imag, own_i, TN)
    )


def base(own, other, total, packed, mine):
    rows, width = own.shape
    return pl.pallas_call(
        base_kernel,
        in_specs=[VMEM] * 5,
        out_specs=[VMEM] * 2,
        out_shape=[jax.ShapeDtypeStruct((rows, width), F32)] * 2,
        cost_estimate=pl.CostEstimate(
            flops=32 * rows * rows * width, bytes_accessed=8 * rows * width, transcendentals=0
        ),
        name="base",
        compiler_params=LIMIT,
    )(own, other, total, packed, mine)


def update_kernel(scale, own_ref, other_ref, base_ref, base_other_ref, theirs_ref, out_ref):
    own, other = own_ref[...], other_ref[...]
    half = own.shape[1] // 2
    own_i, other_i = times_i(own.astype(F32)).astype(BF16), times_i(other.astype(F32)).astype(BF16)
    real, imag = theirs_ref[0], theirs_ref[1]
    product = base_ref[...] + dot(real, other) + dot(imag, other_i)
    product_other = base_other_ref[...] + dot(real, own, TN) - dot(imag, own_i, TN)
    blocks = dot_split(product, product, TN) + dot_split(product_other, product_other, TN)
    real = blocks[:half, :half] + blocks[half:, half:]
    imag = blocks[:half, half:] - blocks[half:, :half]
    diagonal = lax.broadcasted_iota(jnp.int32, (half, 2 * half), 0) == lax.broadcasted_iota(
        jnp.int32, (half, 2 * half), 1
    )
    gram = jnp.concatenate([real, imag], axis=1)
    squares = jnp.sum(jnp.where(diagonal, gram, 0.0))
    size = jnp.full((1, 1), 2.0 * squares / half + 1e-06, F32)
    scaling = lax.rsqrt(size)
    gram = gram * (scaling * scaling)
    identity = jnp.where(diagonal, 1.0, 0.0)
    gram_two = dot_split(gram, complex_stack(gram))
    left = 2.25 * identity - 1.5 * gram + 0.25 * gram_two
    right = 1.5 * gram - 0.5 * gram_two
    factor = 2.25 * identity - 0.75 * gram - 0.5 * dot_split(left, complex_stack(right))
    factor = factor * (scaling * scale)
    out_ref[0] = dot_split(product, complex_stack(factor))


def update(scale, own, other, bases, theirs):
    rows, width = own.shape
    return pl.pallas_call(
        functools.partial(update_kernel, scale),
        in_specs=[VMEM] * 5,
        out_specs=VMEM,
        out_shape=jax.ShapeDtypeStruct((1, rows, width), F32),
        name="update",
        compiler_params=LIMIT,
    )(own, other, *bases, theirs)


def batch_shifts(batch, point_count):
    shifts = {}
    for member in range(BATCH):
        shift = displacement(SHELL_VECTORS[batch * BATCH + member], point_count)
        shifts.setdefault(shift, []).append(member)
    return shifts


def on_device(margins, subspace, shell_weights, window_count):
    point_count = lax.axis_size("kpt")
    side = lax.axis_index("band")
    rows = subspace.shape[1]
    swap = [(0, 1), (1, 0)]
    plan = [batch_shifts(batch, point_count) for batch in range(3)]

    def exchange(value):
        return lax.ppermute(value, "band", swap)

    def fetch(value, shift):
        return lax.ppermute(value, "kpt", fetch_pairs(shift, point_count))

    offset = side * rows
    place = jnp.stack([side, window_count[0] - offset, window_count[0] - (rows - offset)])
    roots = jnp.sqrt(shell_weights)
    own = subspace[0]
    other = exchange(own)
    margins, margin = load(place, margins, SHIPPED)
    margin = exchange(margin)
    halves = {}
    for part, value in (("own", own), ("other", other)):
        for batch in (2, 1):
            for shift in plan[batch]:
                halves[batch, part, shift] = fetch(value, shift)
        for shift in plan[0]:
            near = displacement((shift[0], 0, 1), point_count)
            step = displacement((0, shift[1], -1), point_count)
            halves[0, part, shift] = fetch(halves[1, part, near], step)
    blocks, got = {}, {}
    for batch in (2, 1, 0):
        operands = []
        for shift in plan[batch]:
            operands += [halves[batch, "own", shift], halves[batch, "other", shift]]
        sent = SHIPPED // 2 if batch == 0 else BATCH // 2
        blocks[batch] = project(
            place, roots, margins, batch, list(plan[batch].values()), operands, sent
        )
        got[batch] = exchange(blocks[batch][1])
    operands = []
    for shift, members in plan[0].items():
        if SHIPPED in members or SHIPPED + 1 in members:
            operands += [halves[0, "own", shift], halves[0, "other", shift]]
    got_extra = extra(place, roots, margin, SHIPPED, operands)
    (total,) = gather_own([*blocks[2], *blocks[1]], None)
    total, packed = gather_own(blocks[0], total)
    other_packed = exchange(packed)
    whole = ((0, 0, 1, 0), (0, 1, 1, 1))
    crossed = cross([blocks[2][0], got[2]], whole, None, False)
    crossed = cross(
        [blocks[1][0], got[1], blocks[0][0], got_extra], (*whole, (2, 1, 3, 0)), crossed, False
    )
    mine, theirs = cross([blocks[0][0], got[0]], ((0, 0, 1, 0),), crossed, True)
    theirs = exchange(theirs)
    bases = base(own, other, total, other_packed, mine)
    scale = math.sqrt(rows * lax.axis_size("band"))
    return update(scale, own, other, bases, theirs)


def solution(mesh):
    return jax.shard_map(
        on_device,
        mesh=mesh,
        in_specs=(P("kpt", None, "band", None), P("kpt", "band", None), P(), P("kpt")),
        out_specs=P("kpt", "band", None),
        check_vma=False,
    )
```

```python
import functools
import math

import jax
import jax.numpy as jnp
from jax import lax
from jax.experimental import pallas as pl
from jax.experimental.pallas import tpu as pltpu
from jax.sharding import PartitionSpec as P


SHELL_VECTORS = (
    (1, 1, 0),
    (1, -1, 0),
    (-1, 1, 0),
    (-1, -1, 0),
    (1, 0, 1),
    (1, 0, -1),
    (-1, 0, 1),
    (-1, 0, -1),
    (0, 1, 1),
    (0, 1, -1),
    (0, -1, 1),
    (0, -1, -1),
)
BATCH = 4
SHIPPED = 2
VMEM = pl.BlockSpec(memory_space=pltpu.VMEM)
LIMIT = pltpu.CompilerParams(vmem_limit_bytes=20 * 2**20)
SMEM = pl.BlockSpec(memory_space=pltpu.SMEM)
F32 = jnp.float32
BF16 = jnp.bfloat16
NT = (((1,), (1,)), ((), ()))
TN = (((0,), (0,)), ((), ()))


def grid_shape(point_count):
    size_y = min(4, point_count // 8)
    return (4, size_y, point_count // (4 * size_y))


def displacement(shell, point_count):
    return tuple(step % size for step, size in zip(shell, grid_shape(point_count)))


def fetch_pairs(shift, point_count):
    size_x, size_y, size_z = grid_shape(point_count)
    pairs = []
    for x in range(size_x):
        for y in range(size_y):
            for z in range(size_z):
                source = ((x + shift[0]) % size_x, (y + shift[1]) % size_y, (z + shift[2]) % size_z)
                pairs.append(
                    (
                        (source[0] * size_y + source[1]) * size_z + source[2],
                        (x * size_y + y) * size_z + z,
                    )
                )
    return pairs


def dot(left, right, dims=None):
    if dims is None:
        return jnp.dot(left, right, preferred_element_type=F32)
    return lax.dot_general(left, right, dims, preferred_element_type=F32)


def split(value):
    high = value.astype(BF16)
    return high, (value - high.astype(F32)).astype(BF16)


def dot_exact_right(left, right, dims=None):
    high, low = split(left)
    return dot(high, right, dims) + dot(low, right, dims)


def dot_split(left, right, dims=None):
    left_high, left_low = split(left)
    right_high, right_low = split(right)
    return (
        dot(left_high, right_high, dims)
        + dot(left_high, right_low, dims)
        + dot(left_low, right_high, dims)
    )


def times_minus_i(value):
    half = value.shape[-1] // 2
    return jnp.concatenate([value[:, half:], -value[:, :half]], axis=1)


def times_i(value):
    half = value.shape[-1] // 2
    return jnp.concatenate([-value[:, half:], value[:, :half]], axis=1)


def stack_complex(mine, other, side, rows_ref, stacked_ref):
    rows = mine.shape[0]
    rows_ref[pl.ds(pl.multiple_of(side * rows, 8), rows), :] = mine.astype(F32)
    rows_ref[pl.ds(pl.multiple_of((1 - side) * rows, 8), rows), :] = other.astype(F32)
    whole = rows_ref[...]
    stacked_ref[: 2 * rows, :] = whole.astype(BF16)
    stacked_ref[2 * rows :, :] = times_i(whole).astype(BF16)


def masked_block(margin, stacked, root, limit):
    inside = lax.broadcasted_iota(jnp.int32, (margin.shape[0], 1), 0) < limit
    return jnp.where(inside, dot(margin, stacked) * root, 0.0).astype(BF16)


def project_kernel(groups, first, counts, limit_place, *refs):
    place_ref, root_ref, margins_ref, *refs = refs
    halves = refs[: 2 * len(groups)]
    *out_refs, rows_ref, stacked_ref = refs[2 * len(groups) :]
    side, limit = place_ref[0], place_ref[limit_place]
    for number, members in enumerate(groups):
        mine, other = halves[2 * number][...], halves[2 * number + 1][...]
        stack_complex(mine, other, side, rows_ref, stacked_ref)
        for member in members:
            block = masked_block(
                margins_ref[member], stacked_ref[...], root_ref[first + member], limit
            )
            if member < counts[0]:
                out_refs[0][member] = block
            else:
                out_refs[1][member - counts[0]] = block


def project(place, roots, margins, first, groups, halves, counts, limit_place):
    rows, double = margins.shape[1:]
    width = halves[0].shape[-1]
    return pl.pallas_call(
        functools.partial(project_kernel, groups, first, counts, limit_place),
        in_specs=[SMEM, SMEM, VMEM, *([VMEM] * len(halves))],
        out_specs=[VMEM] * len(counts),
        out_shape=[jax.ShapeDtypeStruct((count, rows, width), BF16) for count in counts],
        scratch_shapes=[pltpu.VMEM((2 * rows, width), F32), pltpu.VMEM((double, width), BF16)],
        cost_estimate=pl.CostEstimate(
            flops=2 * sum(counts) * rows * double * width,
            bytes_accessed=2 * sum(counts) * rows * double,
            transcendentals=0,
        ),
        compiler_params=LIMIT,
    )(place, roots, margins, *halves)


def gather_own_kernel(count, has_total, *refs):
    blocks, refs = refs[:count], refs[count:]
    total_ref = refs[-1]
    rows = blocks[0].shape[1]
    real = jnp.zeros((rows, rows), F32)
    imag = jnp.zeros((rows, rows), F32)
    if has_total:
        real, imag = refs[0][0], refs[0][1]
    for block_ref in blocks:
        for place in range(block_ref.shape[0]):
            block = block_ref[place]
            real += dot(block, block, NT)
            imag += dot(times_minus_i(block), block, NT)
    total_ref[0], total_ref[1] = real, imag


def gather_own(blocks, before):
    rows, width = blocks[0].shape[1:]
    operands = list(blocks) + ([] if before is None else [before])
    return pl.pallas_call(
        functools.partial(gather_own_kernel, len(blocks), before is not None),
        in_specs=[VMEM] * len(operands),
        out_specs=VMEM,
        out_shape=jax.ShapeDtypeStruct((2, rows, rows), F32),
        cost_estimate=pl.CostEstimate(
            flops=8 * len(blocks) * rows * rows * width,
            bytes_accessed=4 * len(blocks) * rows * width,
            transcendentals=0,
        ),
        compiler_params=LIMIT,
    )(*operands)


def add_received(sums, keep_ref, got_ref):
    for place in range(keep_ref.shape[0]):
        keep, got = keep_ref[place], got_ref[place]
        sums[0] += dot(got, got, NT)
        sums[1] += dot(times_minus_i(got), got, NT)
        sums[2] += dot(keep, got, NT)
        sums[3] += dot(times_minus_i(keep), got, NT)
    return sums


def gather_kernel(count, has_total, *refs):
    blocks, refs = refs[: 2 * count], refs[2 * count :]
    total_ref = refs[-1]
    rows = blocks[0].shape[1]
    sums = [jnp.zeros((rows, rows), F32) for _ in range(4)]
    if has_total:
        sums = [refs[0][place] for place in range(4)]
    for place in range(count):
        sums = add_received(sums, blocks[2 * place], blocks[2 * place + 1])
    for place in range(4):
        total_ref[place] = sums[place]


def gather(pairs, before):
    rows, width = pairs[0][0].shape[1:]
    operands = [block for pair in pairs for block in pair] + ([] if before is None else [before])
    terms = sum(pair[0].shape[0] for pair in pairs)
    return pl.pallas_call(
        functools.partial(gather_kernel, len(pairs), before is not None),
        in_specs=[VMEM] * len(operands),
        out_specs=VMEM,
        out_shape=jax.ShapeDtypeStruct((4, rows, rows), F32),
        cost_estimate=pl.CostEstimate(
            flops=8 * terms * rows * rows * width,
            bytes_accessed=4 * terms * rows * width,
            transcendentals=0,
        ),
        compiler_params=LIMIT,
    )(*operands)


def complex_stack(value):
    return jnp.concatenate([value, times_i(value)], axis=0)


def update_kernel(
    scale, own_ref, other_ref, total_ref, before_ref, keep_ref, got_ref, out_ref, sent_ref
):
    own, other = own_ref[...], other_ref[...]
    half = own.shape[1] // 2
    own_i, other_i = times_i(own.astype(F32)).astype(BF16), times_i(other.astype(F32)).astype(BF16)
    sums = add_received([before_ref[place] for place in range(4)], keep_ref, got_ref)
    other_real, other_imag, real, imag = sums
    product = (
        dot_exact_right(total_ref[0], own)
        + dot_exact_right(total_ref[1], own_i)
        + dot_exact_right(real, other)
        + dot_exact_right(imag, other_i)
    )
    product_other = (
        dot_exact_right(other_real, other)
        + dot_exact_right(other_imag, other_i)
        + dot_exact_right(real, own, TN)
        - dot_exact_right(imag, own_i, TN)
    )
    blocks = dot_split(product, product, TN) + dot_split(product_other, product_other, TN)
    real = blocks[:half, :half] + blocks[half:, half:]
    imag = blocks[:half, half:] - blocks[half:, :half]
    diagonal = lax.broadcasted_iota(jnp.int32, (half, 2 * half), 0) == lax.broadcasted_iota(
        jnp.int32, (half, 2 * half), 1
    )
    gram = jnp.concatenate([real, imag], axis=1)
    squares = jnp.sum(jnp.where(diagonal, gram, 0.0))
    size = jnp.full((1, 1), 2.0 * squares / half + 1e-06, F32)
    scaling = lax.rsqrt(size)
    gram = gram * (scaling * scaling)
    identity = jnp.where(diagonal, 1.0, 0.0)
    gram_two = dot_split(gram, complex_stack(gram))
    left = 2.25 * identity - 1.5 * gram + 0.25 * gram_two
    right = 1.5 * gram - 0.5 * gram_two
    factor = 2.25 * identity - 0.75 * gram - 0.5 * dot_split(left, complex_stack(right))
    factor = factor * (scaling * scale)
    factor = complex_stack(factor)
    sent_ref[...] = dot_split(product_other, factor).astype(BF16)
    out_ref[...] = dot_split(product, factor)


def update(scale, own, other, total, before, keep, got):
    rows, width = own.shape
    return pl.pallas_call(
        functools.partial(update_kernel, scale),
        in_specs=[VMEM] * 6,
        out_specs=[VMEM] * 2,
        out_shape=[
            jax.ShapeDtypeStruct((rows, width), F32),
            jax.ShapeDtypeStruct((rows, width), BF16),
        ],
        name="update",
        compiler_params=LIMIT,
    )(own, other, total, before, keep, got)


def batch_shifts(batch, point_count):
    shifts = {}
    for member in range(BATCH):
        shift = displacement(SHELL_VECTORS[batch * BATCH + member], point_count)
        shifts.setdefault(shift, []).append(member)
    return shifts


def on_device(margins, subspace, shell_weights, window_count):
    point_count = lax.axis_size("kpt")
    point_index = lax.axis_index("kpt")
    side = lax.axis_index("band")
    rows = subspace.shape[1]
    plan = [batch_shifts(batch, point_count) for batch in range(3)]

    owner = point_index % 2 == side
    to_owner = [(2 * point + 1 - point % 2, 2 * point + point % 2) for point in range(point_count)]
    from_owner = [(target, source) for source, target in to_owner]

    def give(value, route=to_owner):
        return lax.ppermute(value, ("kpt", "band"), route)

    def fetch(value, shift):
        return lax.ppermute(value, "kpt", fetch_pairs(shift, point_count))

    offset = side * rows
    place = jnp.stack([side, window_count[0] - offset, window_count[0] - (rows - offset)])
    roots = jnp.sqrt(shell_weights)
    own = subspace[0]
    other = lax.ppermute(own, "band", [(0, 1), (1, 0)])
    parts = [margins[0, batch * BATCH : (batch + 1) * BATCH] for batch in range(3)]
    shipped = margins[0, SHIPPED:BATCH]
    shipped = give(shipped)
    halves = {}
    for part, value in (("own", own), ("other", other)):
        for batch in (2, 1):
            for shift in plan[batch]:
                halves[batch, part, shift] = fetch(value, shift)
        for shift in plan[0]:
            near = displacement((shift[0], 0, 1), point_count)
            step = displacement((0, shift[1], -1), point_count)
            halves[0, part, shift] = fetch(halves[1, part, near], step)
    blocks, got, operands = {}, {}, {}
    for batch in (2, 1, 0):
        operands[batch] = []
        for shift in plan[batch]:
            operands[batch] += [halves[batch, "own", shift], halves[batch, "other", shift]]
        blocks[batch] = project(
            place,
            roots,
            parts[batch],
            batch * BATCH,
            list(plan[batch].values()),
            operands[batch],
            (SHIPPED, BATCH - SHIPPED) if batch == 0 else (BATCH,),
            1,
        )
        got[batch] = give(blocks[batch][0])
    groups, near = [], []
    for shift, members in plan[0].items():
        late = [member - SHIPPED for member in members if member >= SHIPPED]
        if late:
            groups.append(late)
            near += [halves[0, "own", shift], halves[0, "other", shift]]
    (got_extra,) = project(place, roots, shipped, SHIPPED, groups, near, (BATCH - SHIPPED,), 2)
    total = gather_own([blocks[2][0], blocks[1][0]], None)
    total = gather_own(blocks[0], total)
    crossed = gather([(blocks[2][0], got[2])], None)
    crossed = gather([(blocks[1][0], got[1]), (blocks[0][1], got_extra)], crossed)
    scale = math.sqrt(rows * lax.axis_size("band"))
    mine, sent = update(scale, own, other, total, crossed, blocks[0][0], got[0])
    theirs = give(sent, from_owner)
    return jnp.where(owner, mine, theirs.astype(F32))[None]


def solution(mesh):
    return jax.shard_map(
        on_device,
        mesh=mesh,
        in_specs=(P("kpt", None, "band", None), P("kpt", "band", None), P(), P("kpt")),
        out_specs=P("kpt", "band", None),
        check_vma=False,
    )
```

```python
import functools
import math

import jax
import jax.numpy as jnp
from jax import lax
from jax.experimental import pallas as pl
from jax.experimental.pallas import tpu as pltpu
from jax.sharding import PartitionSpec as P


SHELL_VECTORS = (
    (1, 1, 0),
    (1, -1, 0),
    (-1, 1, 0),
    (-1, -1, 0),
    (1, 0, 1),
    (1, 0, -1),
    (-1, 0, 1),
    (-1, 0, -1),
    (0, 1, 1),
    (0, 1, -1),
    (0, -1, 1),
    (0, -1, -1),
)
BATCH = 4
SHIPPED = 2
CENTRE = 0.5
PREPARE = 2 * 10**10
VMEM = pl.BlockSpec(memory_space=pltpu.VMEM)
LARGE_LIMIT = pltpu.CompilerParams(vmem_limit_bytes=50 * 2**20)
LIMIT = pltpu.CompilerParams(vmem_limit_bytes=20 * 2**20)
SMEM = pl.BlockSpec(memory_space=pltpu.SMEM)
F32 = jnp.float32
BF16 = jnp.bfloat16
NT = (((1,), (1,)), ((), ()))
TN = (((0,), (0,)), ((), ()))


def grid_shape(point_count):
    size_y = min(4, point_count // 8)
    return (4, size_y, point_count // (4 * size_y))


def displacement(shell, point_count):
    return tuple(step % size for step, size in zip(shell, grid_shape(point_count)))


def fetch_pairs(shift, point_count):
    size_x, size_y, size_z = grid_shape(point_count)
    pairs = []
    for x in range(size_x):
        for y in range(size_y):
            for z in range(size_z):
                source = ((x + shift[0]) % size_x, (y + shift[1]) % size_y, (z + shift[2]) % size_z)
                pairs.append(
                    (
                        (source[0] * size_y + source[1]) * size_z + source[2],
                        (x * size_y + y) * size_z + z,
                    )
                )
    return pairs


def dot(left, right, dims=None):
    if dims is None:
        return jnp.dot(left, right, preferred_element_type=F32)
    return lax.dot_general(left, right, dims, preferred_element_type=F32)


def split(value):
    high = value.astype(BF16)
    return high, (value - high.astype(F32)).astype(BF16)


def dot_exact_right(left, right, dims=None):
    high, low = split(left)
    return dot(high, right, dims) + dot(low, right, dims)


def times_minus_i(value):
    half = value.shape[-1] // 2
    return jnp.concatenate([value[:, half:], -value[:, :half]], axis=1)


def times_i(value):
    half = value.shape[-1] // 2
    return jnp.concatenate([-value[:, half:], value[:, :half]], axis=1)


def stack_complex(mine, other, side, rows_ref, stacked_ref):
    rows = mine.shape[0]
    rows_ref[pl.ds(pl.multiple_of(side * rows, 8), rows), :] = mine.astype(F32)
    rows_ref[pl.ds(pl.multiple_of((1 - side) * rows, 8), rows), :] = other.astype(F32)
    whole = rows_ref[...]
    stacked_ref[: 2 * rows, :] = whole.astype(BF16)
    stacked_ref[2 * rows :, :] = times_i(whole).astype(BF16)


def masked_block(margin, stacked, weight, limit):
    inside = lax.broadcasted_iota(jnp.int32, (margin.shape[0], 1), 0) < limit
    factor = jnp.where(inside, jnp.sqrt(jnp.full((1, 1), weight, F32)), 0.0)
    return (dot(margin, stacked) * factor).astype(BF16)


def prepare_kernel(rows, side_ref, window_ref, out_ref):
    side = side_ref[0]
    out_ref[0] = side
    out_ref[1] = window_ref[0] - side * rows
    out_ref[2] = window_ref[0] - (1 - side) * rows


def prepare(side, window_count, rows):
    return pl.pallas_call(
        functools.partial(prepare_kernel, rows),
        in_specs=[SMEM] * 2,
        out_specs=SMEM,
        out_shape=jax.ShapeDtypeStruct((3,), jnp.int32),
        cost_estimate=pl.CostEstimate(flops=PREPARE, bytes_accessed=64 * 2**20, transcendentals=0),
        name="prepare",
        compiler_params=LIMIT,
    )(side[None], window_count)


def project_kernel(groups, first, sent, streamed, place_ref, weight_ref, margins_ref, *refs):
    halves = refs[: 2 * len(groups)]
    refs = refs[2 * len(groups) :]
    copies = []
    if streamed:
        *refs, fetched_ref, sems = refs
        for member in range(BATCH):
            source = margins_ref.at[0, first + member]
            copies.append(
                pltpu.make_async_copy(source, fetched_ref.at[member], sems.at[member])
            )
            copies[-1].start()
    keep_ref, *give_refs, rows_ref, stacked_ref, blocks_ref = refs
    side, limit = place_ref[0], place_ref[1]
    for number, members in enumerate(groups):
        mine, other = halves[2 * number][...], halves[2 * number + 1][...]
        stack_complex(mine, other, side, rows_ref, stacked_ref)
        for member in members:
            if streamed:
                copies[member].wait()
                margin = fetched_ref[member]
            else:
                margin = margins_ref[0, first + member]
            weight = weight_ref[first + member]
            blocks_ref[member] = masked_block(margin, stacked_ref[...], weight, limit)
    for pair in range(BATCH // 2):
        keep_ref[pair] = blocks_ref[2 * pair + side]
        target = give_refs[0].at[pair] if pair < sent else give_refs[1].at[pair - sent]
        target[...] = blocks_ref[2 * pair + 1 - side]


def project(place, weights, margins, batch, groups, halves, sent, streamed):
    rows, double = margins.shape[2:]
    width = halves[0].shape[-1]
    pairs = BATCH // 2
    counts = [pairs, sent] + ([pairs - sent] if sent < pairs else [])
    streams = []
    if streamed:
        streams = [
            pltpu.VMEM((BATCH, rows, double), BF16),
            pltpu.SemaphoreType.DMA((BATCH,)),
        ]
    return pl.pallas_call(
        functools.partial(project_kernel, groups, batch * BATCH, sent, streamed),
        in_specs=[
            SMEM,
            SMEM,
            pl.BlockSpec(memory_space=pl.ANY) if streamed else VMEM,
            *([VMEM] * len(halves)),
        ],
        out_specs=[VMEM] * len(counts),
        out_shape=[jax.ShapeDtypeStruct((count, rows, width), BF16) for count in counts],
        scratch_shapes=[
            pltpu.VMEM((2 * rows, width), F32),
            pltpu.VMEM((double, width), BF16),
            pltpu.VMEM((BATCH, rows, width), BF16),
            *streams,
        ],
        cost_estimate=pl.CostEstimate(
            flops=2 * BATCH * rows * double * width,
            bytes_accessed=2 * BATCH * rows * double,
            transcendentals=0,
        ),
        compiler_params=LARGE_LIMIT if streamed else LIMIT,
    )(place, weights, margins, *halves)


def extra_kernel(shipped, place_ref, weight_ref, margin_ref, *refs):
    *halves, out_ref, rows_ref, stacked_ref = refs
    side, limit = place_ref[0], place_ref[2]
    mine, other = halves[0][...], halves[1][...]
    if len(halves) > 2:
        mine = jnp.where(side == 0, mine, halves[2][...])
        other = jnp.where(side == 0, other, halves[3][...])
    stack_complex(mine, other, side, rows_ref, stacked_ref)
    weight = weight_ref[shipped + side]
    out_ref[0] = masked_block(margin_ref[...], stacked_ref[...], weight, limit)


def extra(place, weights, margin, shipped, halves):
    rows, double = margin.shape
    width = halves[0].shape[-1]
    return pl.pallas_call(
        functools.partial(extra_kernel, shipped),
        in_specs=[SMEM, SMEM, VMEM, *([VMEM] * len(halves))],
        out_specs=VMEM,
        out_shape=jax.ShapeDtypeStruct((1, rows, width), BF16),
        scratch_shapes=[pltpu.VMEM((2 * rows, width), F32), pltpu.VMEM((double, width), BF16)],
        cost_estimate=pl.CostEstimate(
            flops=2 * rows * double * width, bytes_accessed=2 * rows * double, transcendentals=0
        ),
        name="extra",
        compiler_params=LIMIT,
    )(place, weights, margin, *halves)


def triangle(size):
    row = lax.broadcasted_iota(jnp.int32, (size, size), 0)
    return row, lax.broadcasted_iota(jnp.int32, (size, size), 1)


def gather_own_kernel(count, has_total, *refs):
    blocks, refs = refs[:count], refs[count:]
    rows = blocks[0].shape[1]
    real = jnp.zeros((rows, rows), F32)
    imag = jnp.zeros((rows, rows), F32)
    if has_total:
        real, imag = refs[0][0], refs[0][1]
    for block_ref in blocks:
        for pair in range(block_ref.shape[0]):
            block = block_ref[pair]
            real += dot(block, block, NT)
            imag += dot(times_minus_i(block), block, NT)
    total_ref, *packed = refs[1 if has_total else 0 :]
    total_ref[0], total_ref[1] = real, imag
    if packed:
        row, column = triangle(rows)
        packed[0][...] = jnp.where(row <= column, real, imag).astype(BF16)


def gather_own(blocks, before):
    rows, width = blocks[0].shape[1:]
    count = len(blocks)
    operands = list(blocks) + ([] if before is None else [before])
    results = [jax.ShapeDtypeStruct((2, rows, rows), F32)]
    if before is not None:
        results.append(jax.ShapeDtypeStruct((rows, rows), BF16))
    return pl.pallas_call(
        functools.partial(gather_own_kernel, count, before is not None),
        in_specs=[VMEM] * len(operands),
        out_specs=[VMEM] * len(results),
        out_shape=results,
        cost_estimate=pl.CostEstimate(
            flops=8 * count * rows * rows * width,
            bytes_accessed=4 * count * rows * width,
            transcendentals=0,
        ),
        compiler_params=LIMIT,
    )(*operands)


def cross_kernel(terms, count, has_total, *refs):
    blocks, refs = refs[:count], refs[count:]
    rows = blocks[0].shape[1]
    sums = [jnp.zeros((rows, rows), F32) for _ in range(4)]
    if has_total:
        mine_before_ref, theirs_before_ref, *refs = refs
        sums = [mine_before_ref[0], mine_before_ref[1], theirs_before_ref[0], theirs_before_ref[1]]
    mine_ref, theirs_ref = refs
    for keep_place, keep_index, got_place, got_index in terms:
        keep, got = blocks[keep_place][keep_index], blocks[got_place][got_index]
        sums[0] += dot(keep, got, NT)
        sums[1] += dot(times_minus_i(keep), got, NT)
        sums[2] += dot(got, keep, NT)
        sums[3] += dot(times_minus_i(got), keep, NT)
    mine_ref[0], mine_ref[1] = sums[0], sums[1]
    kind = theirs_ref.dtype
    theirs_ref[0], theirs_ref[1] = sums[2].astype(kind), sums[3].astype(kind)


def cross(blocks, terms, before, last):
    rows, width = blocks[0].shape[1:]
    operands = [*blocks, *(before or ())]
    return pl.pallas_call(
        functools.partial(cross_kernel, terms, len(blocks), before is not None),
        in_specs=[VMEM] * len(operands),
        out_specs=[VMEM] * 2,
        out_shape=[
            jax.ShapeDtypeStruct((2, rows, rows), F32),
            jax.ShapeDtypeStruct((2, rows, rows), BF16 if last else F32),
        ],
        cost_estimate=pl.CostEstimate(
            flops=8 * len(terms) * rows * rows * width,
            bytes_accessed=4 * len(terms) * rows * width,
            transcendentals=0,
        ),
        compiler_params=LIMIT,
    )(*operands)


def dot_complex(left, right):
    stacked = jnp.concatenate([right, times_i(right)], axis=0).astype(BF16)
    return dot(left.astype(BF16), stacked)


def base_kernel(own_ref, other_ref, total_ref, packed_ref, mine_ref, base_ref, base_other_ref):
    own, other = own_ref[...], other_ref[...]
    own_i, other_i = times_i(own.astype(F32)).astype(BF16), times_i(other.astype(F32)).astype(BF16)
    real, imag = mine_ref[0], mine_ref[1]
    base_ref[...] = (
        dot_exact_right(total_ref[0], own)
        + dot_exact_right(total_ref[1], own_i)
        + dot_exact_right(real, other)
        + dot_exact_right(imag, other_i)
    )
    packed = packed_ref[...].astype(F32)
    row, column = triangle(packed.shape[0])
    upper = jnp.where(row <= column, packed, 0.0).astype(BF16)
    strict = jnp.where(row < column, packed, 0.0).astype(BF16)
    lower = jnp.where(row > column, packed, 0.0).astype(BF16)
    base_other_ref[...] = (
        dot(upper, other)
        + dot(strict, other, TN)
        + dot(lower, other_i)
        - dot(lower, other_i, TN)
        + dot_exact_right(real, own, TN)
        - dot_exact_right(imag, own_i, TN)
    )


def base(own, other, total, packed, mine):
    rows, width = own.shape
    return pl.pallas_call(
        base_kernel,
        in_specs=[VMEM] * 5,
        out_specs=[VMEM] * 2,
        out_shape=[jax.ShapeDtypeStruct((rows, width), F32)] * 2,
        cost_estimate=pl.CostEstimate(
            flops=32 * rows * rows * width, bytes_accessed=8 * rows * width, transcendentals=0
        ),
        name="base",
        compiler_params=LIMIT,
    )(own, other, total, packed, mine)


def update_kernel(scale, own_ref, other_ref, base_ref, base_other_ref, theirs_ref, out_ref, rows_ref):
    own, other = own_ref[...], other_ref[...]
    half = own.shape[1] // 2
    own_i, other_i = times_i(own.astype(F32)).astype(BF16), times_i(other.astype(F32)).astype(BF16)
    real, imag = theirs_ref[0], theirs_ref[1]
    rows = own.shape[0]
    product = base_ref[...] + dot(real, other) + dot(imag, other_i)
    rows_ref[:rows, :] = product
    rows_ref[rows:, :] = base_other_ref[...] + dot(real, own, TN) - dot(imag, own_i, TN)
    both = rows_ref[...].astype(BF16)
    blocks = dot(both, both, TN)
    real = blocks[:half, :half] + blocks[half:, half:]
    imag = blocks[:half, half:] - blocks[half:, :half]
    diagonal = lax.broadcasted_iota(jnp.int32, (half, 2 * half), 0) == lax.broadcasted_iota(
        jnp.int32, (half, 2 * half), 1
    )
    gram = jnp.concatenate([real, imag], axis=1)
    squares = jnp.sum(jnp.where(diagonal, gram, 0.0))
    size = jnp.full((1, 1), 2.0 * squares / half + 1e-06, F32)
    scaling = lax.rsqrt(size)
    rest = gram * (scaling * scaling) - jnp.where(diagonal, CENTRE, 0.0)
    square = 2.0 * CENTRE * rest + dot_complex(rest, rest)
    left_centre = 2.25 - 1.5 * CENTRE + 0.25 * CENTRE**2
    right_centre = 1.5 * CENTRE - 0.5 * CENTRE**2
    left = 0.25 * square - 1.5 * rest
    right = 1.5 * rest - 0.5 * square
    both_sides = left_centre * right + right_centre * left + dot_complex(left, right)
    factor = -0.75 * rest - 0.5 * both_sides
    centre = 2.25 - 0.75 * CENTRE - 0.5 * left_centre * right_centre
    out_ref[0] = (product * centre + dot_complex(product, factor)) * (scaling * scale)


def update(scale, own, other, bases, theirs):
    rows, width = own.shape
    return pl.pallas_call(
        functools.partial(update_kernel, scale),
        in_specs=[VMEM] * 5,
        out_specs=VMEM,
        out_shape=jax.ShapeDtypeStruct((1, rows, width), F32),
        scratch_shapes=[pltpu.VMEM((2 * rows, width), F32)],
        name="update",
        compiler_params=LIMIT,
    )(own, other, *bases, theirs)


def batch_shifts(batch, point_count):
    shifts = {}
    for member in range(BATCH):
        shift = displacement(SHELL_VECTORS[batch * BATCH + member], point_count)
        shifts.setdefault(shift, []).append(member)
    return shifts


def on_device(margins, subspace, shell_weights, window_count):
    point_count = lax.axis_size("kpt")
    side = lax.axis_index("band")
    rows = subspace.shape[1]
    swap = [(0, 1), (1, 0)]
    plan = [batch_shifts(batch, point_count) for batch in range(3)]

    def exchange(value):
        return lax.ppermute(value, "band", swap)

    def fetch(value, shift):
        return lax.ppermute(value, "kpt", fetch_pairs(shift, point_count))

    place = prepare(side, window_count, rows)
    own = subspace[0]
    other = exchange(own)
    margin = lax.dynamic_index_in_dim(margins[0], SHIPPED + 1 - side, 0, keepdims=False)
    margin = exchange(margin)
    halves = {}
    for part, value in (("own", own), ("other", other)):
        for batch in (2, 1):
            for shift in plan[batch]:
                halves[batch, part, shift] = fetch(value, shift)
        for shift in plan[0]:
            near = displacement((shift[0], 0, 1), point_count)
            step = displacement((0, shift[1], -1), point_count)
            halves[0, part, shift] = fetch(halves[1, part, near], step)
    blocks, got = {}, {}
    for batch in (2, 1, 0):
        operands = []
        for shift in plan[batch]:
            operands += [halves[batch, "own", shift], halves[batch, "other", shift]]
        sent = SHIPPED // 2 if batch == 0 else BATCH // 2
        blocks[batch] = project(
            place, shell_weights, margins, batch, list(plan[batch].values()), operands, sent, False
        )
        got[batch] = exchange(blocks[batch][1])
    operands = []
    for shift, members in plan[0].items():
        if SHIPPED in members or SHIPPED + 1 in members:
            operands += [halves[0, "own", shift], halves[0, "other", shift]]
    got_extra = extra(place, shell_weights, margin, SHIPPED, operands)
    (total,) = gather_own([*blocks[2], *blocks[1]], None)
    total, packed = gather_own(blocks[0], total)
    other_packed = exchange(packed)
    whole = ((0, 0, 1, 0), (0, 1, 1, 1))
    crossed = cross([blocks[2][0], got[2]], whole, None, False)
    crossed = cross(
        [blocks[1][0], got[1], blocks[0][0], got_extra], (*whole, (2, 1, 3, 0)), crossed, False
    )
    mine, theirs = cross([blocks[0][0], got[0]], ((0, 0, 1, 0),), crossed, True)
    theirs = exchange(theirs)
    bases = base(own, other, total, other_packed, mine)
    scale = math.sqrt(rows * lax.axis_size("band"))
    return update(scale, own, other, bases, theirs)


def solution(mesh):
    return jax.shard_map(
        on_device,
        mesh=mesh,
        in_specs=(P("kpt", None, "band", None), P("kpt", "band", None), P(), P("kpt")),
        out_specs=P("kpt", "band", None),
        check_vma=False,
    )
```

```python
import functools
import math

import jax
import jax.numpy as jnp
from jax import lax
from jax.experimental import pallas as pl
from jax.experimental.pallas import tpu as pltpu
from jax.sharding import PartitionSpec as P


SHELL_VECTORS = (
    (1, 1, 0),
    (1, -1, 0),
    (-1, 1, 0),
    (-1, -1, 0),
    (1, 0, 1),
    (1, 0, -1),
    (-1, 0, 1),
    (-1, 0, -1),
    (0, 1, 1),
    (0, 1, -1),
    (0, -1, 1),
    (0, -1, -1),
)
BATCH = 4
SHIPPED = 2
CENTRE = 0.5
PREPARE = 2 * 10**10
VMEM = pl.BlockSpec(memory_space=pltpu.VMEM)
LARGE_LIMIT = pltpu.CompilerParams(vmem_limit_bytes=50 * 2**20)
LIMIT = pltpu.CompilerParams(vmem_limit_bytes=20 * 2**20)
SMEM = pl.BlockSpec(memory_space=pltpu.SMEM)
F32 = jnp.float32
BF16 = jnp.bfloat16
NT = (((1,), (1,)), ((), ()))
TN = (((0,), (0,)), ((), ()))


def grid_shape(point_count):
    size_y = min(4, point_count // 8)
    return (4, size_y, point_count // (4 * size_y))


def displacement(shell, point_count):
    return tuple(step % size for step, size in zip(shell, grid_shape(point_count)))


def fetch_pairs(shift, point_count):
    size_x, size_y, size_z = grid_shape(point_count)
    pairs = []
    for x in range(size_x):
        for y in range(size_y):
            for z in range(size_z):
                source = ((x + shift[0]) % size_x, (y + shift[1]) % size_y, (z + shift[2]) % size_z)
                pairs.append(
                    (
                        (source[0] * size_y + source[1]) * size_z + source[2],
                        (x * size_y + y) * size_z + z,
                    )
                )
    return pairs


def dot(left, right, dims=None):
    if dims is None:
        return jnp.dot(left, right, preferred_element_type=F32)
    return lax.dot_general(left, right, dims, preferred_element_type=F32)


def split(value):
    high = value.astype(BF16)
    return high, (value - high.astype(F32)).astype(BF16)


def dot_exact_right(left, right, dims=None):
    high, low = split(left)
    return dot(high, right, dims) + dot(low, right, dims)


def times_minus_i(value):
    half = value.shape[-1] // 2
    return jnp.concatenate([value[:, half:], -value[:, :half]], axis=1)


def times_i(value):
    half = value.shape[-1] // 2
    return jnp.concatenate([-value[:, half:], value[:, :half]], axis=1)


def stack_complex(mine, other, side, rows_ref, stacked_ref):
    rows = mine.shape[0]
    rows_ref[pl.ds(pl.multiple_of(side * rows, 8), rows), :] = mine.astype(F32)
    rows_ref[pl.ds(pl.multiple_of((1 - side) * rows, 8), rows), :] = other.astype(F32)
    whole = rows_ref[...]
    stacked_ref[: 2 * rows, :] = whole.astype(BF16)
    stacked_ref[2 * rows :, :] = times_i(whole).astype(BF16)


def masked_block(margin, stacked, weight, limit):
    inside = lax.broadcasted_iota(jnp.int32, (margin.shape[0], 1), 0) < limit
    factor = jnp.where(inside, jnp.sqrt(jnp.full((1, 1), weight, F32)), 0.0)
    return (dot(margin, stacked) * factor).astype(BF16)


def prepare_kernel(rows, side_ref, window_ref, out_ref):
    side = side_ref[0]
    out_ref[0] = side
    out_ref[1] = window_ref[0] - side * rows
    out_ref[2] = window_ref[0] - (1 - side) * rows


def prepare(side, window_count, rows):
    return pl.pallas_call(
        functools.partial(prepare_kernel, rows),
        in_specs=[SMEM] * 2,
        out_specs=SMEM,
        out_shape=jax.ShapeDtypeStruct((3,), jnp.int32),
        cost_estimate=pl.CostEstimate(flops=PREPARE, bytes_accessed=64 * 2**20, transcendentals=0),
        name="prepare",
        compiler_params=LIMIT,
    )(side[None], window_count)


def project_kernel(groups, first, sent, streamed, place_ref, weight_ref, margins_ref, *refs):
    halves = refs[: 2 * len(groups)]
    refs = refs[2 * len(groups) :]
    copies = []
    if streamed:
        *refs, fetched_ref, sems = refs
        for member in range(BATCH):
            source = margins_ref.at[0, first + member]
            copies.append(
                pltpu.make_async_copy(source, fetched_ref.at[member], sems.at[member])
            )
            copies[-1].start()
    keep_ref, *give_refs, rows_ref, stacked_ref, blocks_ref = refs
    side, limit = place_ref[0], place_ref[1]
    for number, members in enumerate(groups):
        mine, other = halves[2 * number][...], halves[2 * number + 1][...]
        stack_complex(mine, other, side, rows_ref, stacked_ref)
        for member in members:
            if streamed:
                copies[member].wait()
                margin = fetched_ref[member]
            else:
                margin = margins_ref[0, first + member]
            weight = weight_ref[first + member]
            blocks_ref[member] = masked_block(margin, stacked_ref[...], weight, limit)
    for pair in range(BATCH // 2):
        keep_ref[pair] = blocks_ref[2 * pair + side]
        target = give_refs[0].at[pair] if pair < sent else give_refs[1].at[pair - sent]
        target[...] = blocks_ref[2 * pair + 1 - side]


def project(place, weights, margins, batch, groups, halves, sent, streamed):
    rows, double = margins.shape[2:]
    width = halves[0].shape[-1]
    pairs = BATCH // 2
    counts = [pairs, sent] + ([pairs - sent] if sent < pairs else [])
    streams = []
    if streamed:
        streams = [
            pltpu.VMEM((BATCH, rows, double), BF16),
            pltpu.SemaphoreType.DMA((BATCH,)),
        ]
    return pl.pallas_call(
        functools.partial(project_kernel, groups, batch * BATCH, sent, streamed),
        in_specs=[
            SMEM,
            SMEM,
            pl.BlockSpec(memory_space=pl.ANY) if streamed else VMEM,
            *([VMEM] * len(halves)),
        ],
        out_specs=[VMEM] * len(counts),
        out_shape=[jax.ShapeDtypeStruct((count, rows, width), BF16) for count in counts],
        scratch_shapes=[
            pltpu.VMEM((2 * rows, width), F32),
            pltpu.VMEM((double, width), BF16),
            pltpu.VMEM((BATCH, rows, width), BF16),
            *streams,
        ],
        cost_estimate=pl.CostEstimate(
            flops=2 * BATCH * rows * double * width,
            bytes_accessed=2 * BATCH * rows * double,
            transcendentals=0,
        ),
        compiler_params=LARGE_LIMIT if streamed else LIMIT,
    )(place, weights, margins, *halves)


def extra_kernel(shipped, place_ref, weight_ref, margin_ref, *refs):
    *halves, out_ref, rows_ref, stacked_ref = refs
    side, limit = place_ref[0], place_ref[2]
    mine, other = halves[0][...], halves[1][...]
    if len(halves) > 2:
        mine = jnp.where(side == 0, mine, halves[2][...])
        other = jnp.where(side == 0, other, halves[3][...])
    stack_complex(mine, other, side, rows_ref, stacked_ref)
    weight = weight_ref[shipped + side]
    out_ref[0] = masked_block(margin_ref[...], stacked_ref[...], weight, limit)


def extra(place, weights, margin, shipped, halves):
    rows, double = margin.shape
    width = halves[0].shape[-1]
    return pl.pallas_call(
        functools.partial(extra_kernel, shipped),
        in_specs=[SMEM, SMEM, VMEM, *([VMEM] * len(halves))],
        out_specs=VMEM,
        out_shape=jax.ShapeDtypeStruct((1, rows, width), BF16),
        scratch_shapes=[pltpu.VMEM((2 * rows, width), F32), pltpu.VMEM((double, width), BF16)],
        cost_estimate=pl.CostEstimate(
            flops=2 * rows * double * width, bytes_accessed=2 * rows * double, transcendentals=0
        ),
        name="extra",
        compiler_params=LIMIT,
    )(place, weights, margin, *halves)


def triangle(size):
    row = lax.broadcasted_iota(jnp.int32, (size, size), 0)
    return row, lax.broadcasted_iota(jnp.int32, (size, size), 1)


def gather_own_kernel(count, has_total, *refs):
    blocks, refs = refs[:count], refs[count:]
    rows = blocks[0].shape[1]
    real = jnp.zeros((rows, rows), F32)
    imag = jnp.zeros((rows, rows), F32)
    if has_total:
        real, imag = refs[0][0], refs[0][1]
    for block_ref in blocks:
        for pair in range(block_ref.shape[0]):
            block = block_ref[pair]
            real += dot(block, block, NT)
            imag += dot(times_minus_i(block), block, NT)
    total_ref, *packed = refs[1 if has_total else 0 :]
    total_ref[0], total_ref[1] = real, imag
    if packed:
        row, column = triangle(rows)
        packed[0][...] = jnp.where(row <= column, real, imag).astype(BF16)


def gather_own(blocks, before):
    rows, width = blocks[0].shape[1:]
    count = len(blocks)
    operands = list(blocks) + ([] if before is None else [before])
    results = [jax.ShapeDtypeStruct((2, rows, rows), F32)]
    if before is not None:
        results.append(jax.ShapeDtypeStruct((rows, rows), BF16))
    return pl.pallas_call(
        functools.partial(gather_own_kernel, count, before is not None),
        in_specs=[VMEM] * len(operands),
        out_specs=[VMEM] * len(results),
        out_shape=results,
        cost_estimate=pl.CostEstimate(
            flops=8 * count * rows * rows * width,
            bytes_accessed=4 * count * rows * width,
            transcendentals=0,
        ),
        compiler_params=LIMIT,
    )(*operands)


def cross_kernel(terms, count, has_total, *refs):
    blocks, refs = refs[:count], refs[count:]
    rows = blocks[0].shape[1]
    sums = [jnp.zeros((rows, rows), F32) for _ in range(4)]
    if has_total:
        mine_before_ref, theirs_before_ref, *refs = refs
        sums = [mine_before_ref[0], mine_before_ref[1], theirs_before_ref[0], theirs_before_ref[1]]
    mine_ref, theirs_ref = refs
    for keep_place, keep_index, got_place, got_index in terms:
        keep, got = blocks[keep_place][keep_index], blocks[got_place][got_index]
        sums[0] += dot(keep, got, NT)
        sums[1] += dot(times_minus_i(keep), got, NT)
        sums[2] += dot(got, keep, NT)
        sums[3] += dot(times_minus_i(got), keep, NT)
    mine_ref[0], mine_ref[1] = sums[0], sums[1]
    kind = theirs_ref.dtype
    theirs_ref[0], theirs_ref[1] = sums[2].astype(kind), sums[3].astype(kind)


def cross(blocks, terms, before, last):
    rows, width = blocks[0].shape[1:]
    operands = [*blocks, *(before or ())]
    return pl.pallas_call(
        functools.partial(cross_kernel, terms, len(blocks), before is not None),
        in_specs=[VMEM] * len(operands),
        out_specs=[VMEM] * 2,
        out_shape=[
            jax.ShapeDtypeStruct((2, rows, rows), F32),
            jax.ShapeDtypeStruct((2, rows, rows), BF16 if last else F32),
        ],
        cost_estimate=pl.CostEstimate(
            flops=8 * len(terms) * rows * rows * width,
            bytes_accessed=4 * len(terms) * rows * width,
            transcendentals=0,
        ),
        compiler_params=LIMIT,
    )(*operands)


def dot_complex(left, right):
    stacked = jnp.concatenate([right, times_i(right)], axis=0).astype(BF16)
    return dot(left.astype(BF16), stacked)


def base_kernel(own_ref, other_ref, total_ref, packed_ref, mine_ref, base_ref, base_other_ref):
    own, other = own_ref[...], other_ref[...]
    own_i, other_i = times_i(own.astype(F32)).astype(BF16), times_i(other.astype(F32)).astype(BF16)
    real, imag = mine_ref[0], mine_ref[1]
    base_ref[...] = (
        dot_exact_right(total_ref[0], own)
        + dot_exact_right(total_ref[1], own_i)
        + dot_exact_right(real, other)
        + dot_exact_right(imag, other_i)
    )
    packed = packed_ref[...].astype(F32)
    row, column = triangle(packed.shape[0])
    upper = jnp.where(row <= column, packed, 0.0).astype(BF16)
    strict = jnp.where(row < column, packed, 0.0).astype(BF16)
    lower = jnp.where(row > column, packed, 0.0).astype(BF16)
    base_other_ref[...] = (
        dot(upper, other)
        + dot(strict, other, TN)
        + dot(lower, other_i)
        - dot(lower, other_i, TN)
        + dot_exact_right(real, own, TN)
        - dot_exact_right(imag, own_i, TN)
    )


def base(own, other, total, packed, mine):
    rows, width = own.shape
    return pl.pallas_call(
        base_kernel,
        in_specs=[VMEM] * 5,
        out_specs=[VMEM] * 2,
        out_shape=[jax.ShapeDtypeStruct((rows, width), F32)] * 2,
        cost_estimate=pl.CostEstimate(
            flops=32 * rows * rows * width, bytes_accessed=8 * rows * width, transcendentals=0
        ),
        name="base",
        compiler_params=LIMIT,
    )(own, other, total, packed, mine)


def update_kernel(scale, own_ref, other_ref, base_ref, base_other_ref, theirs_ref, out_ref, rows_ref):
    own, other = own_ref[...], other_ref[...]
    half = own.shape[1] // 2
    own_i, other_i = times_i(own.astype(F32)).astype(BF16), times_i(other.astype(F32)).astype(BF16)
    real, imag = theirs_ref[0], theirs_ref[1]
    rows = own.shape[0]
    product = base_ref[...] + dot(real, other) + dot(imag, other_i)
    rows_ref[:rows, :] = product
    rows_ref[rows:, :] = base_other_ref[...] + dot(real, own, TN) - dot(imag, own_i, TN)
    both = rows_ref[...].astype(BF16)
    blocks = dot(both, both, TN)
    real = blocks[:half, :half] + blocks[half:, half:]
    imag = blocks[:half, half:] - blocks[half:, :half]
    diagonal = lax.broadcasted_iota(jnp.int32, (half, 2 * half), 0) == lax.broadcasted_iota(
        jnp.int32, (half, 2 * half), 1
    )
    gram = jnp.concatenate([real, imag], axis=1)
    squares = jnp.sum(jnp.where(diagonal, gram, 0.0))
    size = jnp.full((1, 1), 2.0 * squares / half + 1e-06, F32)
    scaling = lax.rsqrt(size)
    rest = gram * (scaling * scaling) - jnp.where(diagonal, CENTRE, 0.0)
    square = 2.0 * CENTRE * rest + dot_complex(rest, rest)
    left_centre = 2.25 - 1.5 * CENTRE + 0.25 * CENTRE**2
    right_centre = 1.5 * CENTRE - 0.5 * CENTRE**2
    left = 0.25 * square - 1.5 * rest
    right = 1.5 * rest - 0.5 * square
    both_sides = left_centre * right + right_centre * left + dot_complex(left, right)
    factor = -0.75 * rest - 0.5 * both_sides
    centre = 2.25 - 0.75 * CENTRE - 0.5 * left_centre * right_centre
    stacked = jnp.concatenate([factor, times_i(factor)], axis=0)
    high, low = split(product)
    stacked_high, stacked_low = split(stacked)
    change = dot(high, stacked_high) + dot(low, stacked_high) + dot(high, stacked_low)
    out_ref[0] = (product * centre + change) * (scaling * scale)


def update(scale, own, other, bases, theirs):
    rows, width = own.shape
    return pl.pallas_call(
        functools.partial(update_kernel, scale),
        in_specs=[VMEM] * 5,
        out_specs=VMEM,
        out_shape=jax.ShapeDtypeStruct((1, rows, width), F32),
        scratch_shapes=[pltpu.VMEM((2 * rows, width), F32)],
        name="update",
        compiler_params=LIMIT,
    )(own, other, *bases, theirs)


def batch_shifts(batch, point_count):
    shifts = {}
    for member in range(BATCH):
        shift = displacement(SHELL_VECTORS[batch * BATCH + member], point_count)
        shifts.setdefault(shift, []).append(member)
    return shifts


def on_device(margins, subspace, shell_weights, window_count):
    point_count = lax.axis_size("kpt")
    side = lax.axis_index("band")
    rows = subspace.shape[1]
    swap = [(0, 1), (1, 0)]
    plan = [batch_shifts(batch, point_count) for batch in range(3)]

    def exchange(value):
        return lax.ppermute(value, "band", swap)

    def fetch(value, shift):
        return lax.ppermute(value, "kpt", fetch_pairs(shift, point_count))

    place = prepare(side, window_count, rows)
    own = subspace[0]
    other = exchange(own)
    margin = lax.dynamic_index_in_dim(margins[0], SHIPPED + 1 - side, 0, keepdims=False)
    margin = exchange(margin)
    halves = {}
    for part, value in (("own", own), ("other", other)):
        for batch in (2, 1):
            for shift in plan[batch]:
                halves[batch, part, shift] = fetch(value, shift)
        for shift in plan[0]:
            near = displacement((shift[0], 0, 1), point_count)
            step = displacement((0, shift[1], -1), point_count)
            halves[0, part, shift] = fetch(halves[1, part, near], step)
    blocks, got = {}, {}
    for batch in (2, 1, 0):
        operands = []
        for shift in plan[batch]:
            operands += [halves[batch, "own", shift], halves[batch, "other", shift]]
        sent = SHIPPED // 2 if batch == 0 else BATCH // 2
        blocks[batch] = project(
            place, shell_weights, margins, batch, list(plan[batch].values()), operands, sent, False
        )
        got[batch] = exchange(blocks[batch][1])
    operands = []
    for shift, members in plan[0].items():
        if SHIPPED in members or SHIPPED + 1 in members:
            operands += [halves[0, "own", shift], halves[0, "other", shift]]
    got_extra = extra(place, shell_weights, margin, SHIPPED, operands)
    (total,) = gather_own([*blocks[2], *blocks[1]], None)
    total, packed = gather_own(blocks[0], total)
    other_packed = exchange(packed)
    whole = ((0, 0, 1, 0), (0, 1, 1, 1))
    crossed = cross([blocks[2][0], got[2]], whole, None, False)
    crossed = cross(
        [blocks[1][0], got[1], blocks[0][0], got_extra], (*whole, (2, 1, 3, 0)), crossed, False
    )
    mine, theirs = cross([blocks[0][0], got[0]], ((0, 0, 1, 0),), crossed, True)
    theirs = exchange(theirs)
    bases = base(own, other, total, other_packed, mine)
    scale = math.sqrt(rows * lax.axis_size("band"))
    return update(scale, own, other, bases, theirs)


def solution(mesh):
    return jax.shard_map(
        on_device,
        mesh=mesh,
        in_specs=(P("kpt", None, "band", None), P("kpt", "band", None), P(), P("kpt")),
        out_specs=P("kpt", "band", None),
        check_vma=False,
    )
```

```python
import functools
import math

import jax
import jax.numpy as jnp
from jax import lax
from jax.experimental import pallas as pl
from jax.experimental.pallas import tpu as pltpu
from jax.sharding import PartitionSpec as P


SHELL_VECTORS = (
    (1, 1, 0),
    (1, -1, 0),
    (-1, 1, 0),
    (-1, -1, 0),
    (1, 0, 1),
    (1, 0, -1),
    (-1, 0, 1),
    (-1, 0, -1),
    (0, 1, 1),
    (0, 1, -1),
    (0, -1, 1),
    (0, -1, -1),
)
BATCH = 4
SHIPPED = 2
CENTRE = 0.5
PREPARE = 2 * 10**10
VMEM = pl.BlockSpec(memory_space=pltpu.VMEM)
LIMIT = pltpu.CompilerParams(vmem_limit_bytes=20 * 2**20)
SMEM = pl.BlockSpec(memory_space=pltpu.SMEM)
F32 = jnp.float32
BF16 = jnp.bfloat16
NT = (((1,), (1,)), ((), ()))
TN = (((0,), (0,)), ((), ()))


def grid_shape(point_count):
    size_y = min(4, point_count // 8)
    return (4, size_y, point_count // (4 * size_y))


def displacement(shell, point_count):
    return tuple(step % size for step, size in zip(shell, grid_shape(point_count)))


def fetch_pairs(shift, point_count):
    size_x, size_y, size_z = grid_shape(point_count)
    pairs = []
    for x in range(size_x):
        for y in range(size_y):
            for z in range(size_z):
                source = ((x + shift[0]) % size_x, (y + shift[1]) % size_y, (z + shift[2]) % size_z)
                pairs.append(
                    (
                        (source[0] * size_y + source[1]) * size_z + source[2],
                        (x * size_y + y) * size_z + z,
                    )
                )
    return pairs


def dot(left, right, dims=None):
    if dims is None:
        return jnp.dot(left, right, preferred_element_type=F32)
    return lax.dot_general(left, right, dims, preferred_element_type=F32)


def split(value):
    high = value.astype(BF16)
    return high, (value - high.astype(F32)).astype(BF16)


def dot_exact_right(left, right, dims=None):
    high, low = split(left)
    return dot(high, right, dims) + dot(low, right, dims)


def times_minus_i(value):
    half = value.shape[-1] // 2
    return jnp.concatenate([value[:, half:], -value[:, :half]], axis=1)


def times_i(value):
    half = value.shape[-1] // 2
    return jnp.concatenate([-value[:, half:], value[:, :half]], axis=1)


def stack_complex(mine, other, side, rows_ref, stacked_ref):
    rows = mine.shape[0]
    rows_ref[pl.ds(pl.multiple_of(side * rows, 8), rows), :] = mine.astype(F32)
    rows_ref[pl.ds(pl.multiple_of((1 - side) * rows, 8), rows), :] = other.astype(F32)
    whole = rows_ref[...]
    stacked_ref[: 2 * rows, :] = whole.astype(BF16)
    stacked_ref[2 * rows :, :] = times_i(whole).astype(BF16)


def masked_blocks(margins, stacked, weights, limit):
    count, rows, double = margins.shape
    inside = lax.broadcasted_iota(jnp.int32, (rows, 1), 0) < limit
    products = dot(margins.reshape(count * rows, double), stacked)
    blocks = []
    for place, weight in enumerate(weights):
        factor = jnp.where(inside, jnp.sqrt(jnp.full((1, 1), weight, F32)), 0.0)
        blocks.append((products[place * rows : (place + 1) * rows] * factor).astype(BF16))
    return blocks


def prepare_kernel(out_ref):
    out_ref[...] = jnp.zeros_like(out_ref)


def prepare():
    return pl.pallas_call(
        prepare_kernel,
        out_specs=VMEM,
        out_shape=jax.ShapeDtypeStruct((8, 128), jnp.int32),
        cost_estimate=pl.CostEstimate(flops=PREPARE, bytes_accessed=2**26, transcendentals=0),
        name="prepare",
        compiler_params=LIMIT,
    )()


def project_kernel(groups, first, sent, side_ref, window_ref, weight_ref, margins_ref, *refs):
    halves = refs[: 2 * len(groups)]
    *out_refs, rows_ref, stacked_ref, blocks_ref = refs[2 * len(groups) :]
    shipped_ref = None
    if not sent:
        shipped_ref, keep_ref, other_ref, got_ref = out_refs
    else:
        _, keep_ref, other_ref = out_refs
    side = side_ref[0]
    rows = margins_ref.shape[2]
    limits = [window_ref[...] - side * rows, window_ref[...] - (1 - side) * rows]
    for number, members in enumerate(groups):
        mine, other = halves[2 * number][...], halves[2 * number + 1][...]
        stack_complex(mine, other, side, rows_ref, stacked_ref)
        start, count = first + members[0], len(members)
        blocks = masked_blocks(
            margins_ref[0, start : start + count],
            stacked_ref[...],
            [weight_ref[first + member] for member in members],
            limits[0],
        )
        for member, block in zip(members, blocks):
            blocks_ref[member] = block
            if not sent:
                @pl.when(side == member % 2)
                def _():
                    weight = weight_ref[first + member]
                    (got_ref[0],) = masked_blocks(
                        shipped_ref[...][None], stacked_ref[...], [weight], limits[1]
                    )
    for pair in range(keep_ref.shape[0]):
        keep_ref[pair] = blocks_ref[2 * pair + side]
        other_ref[pair] = blocks_ref[2 * pair + 1 - side]


def project(place, weights, margins, first, groups, halves, extra, sent):
    rows, double = margins.shape[2:]
    width = halves[0].shape[-1]
    members = sum(len(group) for group in groups)
    counts = [members // 2, members // 2] + ([] if sent else [1])
    return pl.pallas_call(
        functools.partial(project_kernel, groups, first, sent),
        in_specs=[SMEM, VMEM, SMEM, VMEM, *([VMEM] * len(halves)), VMEM],
        out_specs=[VMEM] * len(counts),
        out_shape=[jax.ShapeDtypeStruct((count, rows, width), BF16) for count in counts],
        scratch_shapes=[
            pltpu.VMEM((2 * rows, width), F32),
            pltpu.VMEM((double, width), BF16),
            pltpu.VMEM((members, rows, width), BF16),
        ],
        cost_estimate=pl.CostEstimate(
            flops=2 * members * rows * double * width,
            bytes_accessed=2 * members * rows * double,
            transcendentals=0,
        ),
        compiler_params=LIMIT,
    )(*place, weights, margins, *halves, extra)


def triangle(size):
    row = lax.broadcasted_iota(jnp.int32, (size, size), 0)
    return row, lax.broadcasted_iota(jnp.int32, (size, size), 1)


def gather_own_kernel(count, has_total, *refs):
    blocks, refs = refs[:count], refs[count:]
    rows = blocks[0].shape[1]
    real = jnp.zeros((rows, rows), F32)
    imag = jnp.zeros((rows, rows), F32)
    if has_total:
        real, imag = refs[0][0], refs[0][1]
    for block_ref in blocks:
        for pair in range(block_ref.shape[0]):
            block = block_ref[pair]
            real += dot(block, block, NT)
            imag += dot(times_minus_i(block), block, NT)
    total_ref, *packed = refs[1 if has_total else 0 :]
    total_ref[0], total_ref[1] = real, imag
    if packed:
        row, column = triangle(rows)
        packed[0][...] = jnp.where(row <= column, real, imag).astype(BF16)


def gather_own(blocks, before):
    rows, width = blocks[0].shape[1:]
    count = len(blocks)
    operands = list(blocks) + ([] if before is None else [before])
    results = [jax.ShapeDtypeStruct((2, rows, rows), F32)]
    if before is not None:
        results.append(jax.ShapeDtypeStruct((rows, rows), BF16))
    return pl.pallas_call(
        functools.partial(gather_own_kernel, count, before is not None),
        in_specs=[VMEM] * len(operands),
        out_specs=[VMEM] * len(results),
        out_shape=results,
        cost_estimate=pl.CostEstimate(
            flops=8 * count * rows * rows * width,
            bytes_accessed=4 * count * rows * width,
            transcendentals=0,
        ),
        compiler_params=LIMIT,
    )(*operands)


def cross_kernel(terms, count, has_total, *refs):
    blocks, refs = refs[:count], refs[count:]
    rows = blocks[0].shape[1]
    sums = [jnp.zeros((rows, rows), F32) for _ in range(4)]
    if has_total:
        mine_before_ref, theirs_before_ref, *refs = refs
        sums = [mine_before_ref[0], mine_before_ref[1], theirs_before_ref[0], theirs_before_ref[1]]
    mine_ref, theirs_ref = refs
    for keep_place, keep_index, got_place, got_index in terms:
        keep, got = blocks[keep_place][keep_index], blocks[got_place][got_index]
        sums[0] += dot(keep, got, NT)
        sums[1] += dot(times_minus_i(keep), got, NT)
        sums[2] += dot(got, keep, NT)
        sums[3] += dot(times_minus_i(got), keep, NT)
    mine_ref[0], mine_ref[1] = sums[0], sums[1]
    kind = theirs_ref.dtype
    theirs_ref[0], theirs_ref[1] = sums[2].astype(kind), sums[3].astype(kind)


def cross(blocks, terms, before, last):
    rows, width = blocks[0].shape[1:]
    operands = [*blocks, *(before or ())]
    return pl.pallas_call(
        functools.partial(cross_kernel, terms, len(blocks), before is not None),
        in_specs=[VMEM] * len(operands),
        out_specs=[VMEM] * 2,
        out_shape=[
            jax.ShapeDtypeStruct((2, rows, rows), F32),
            jax.ShapeDtypeStruct((2, rows, rows), BF16 if last else F32),
        ],
        cost_estimate=pl.CostEstimate(
            flops=8 * len(terms) * rows * rows * width,
            bytes_accessed=4 * len(terms) * rows * width,
            transcendentals=0,
        ),
        compiler_params=LIMIT,
    )(*operands)


def dot_complex(left, right):
    stacked = jnp.concatenate([right, times_i(right)], axis=0).astype(BF16)
    return dot(left.astype(BF16), stacked)


def base_kernel(own_ref, other_ref, total_ref, packed_ref, mine_ref, base_ref, base_other_ref):
    own, other = own_ref[...], other_ref[...]
    own_i, other_i = times_i(own.astype(F32)).astype(BF16), times_i(other.astype(F32)).astype(BF16)
    real, imag = mine_ref[0], mine_ref[1]
    base_ref[...] = (
        dot_exact_right(total_ref[0], own)
        + dot_exact_right(total_ref[1], own_i)
        + dot_exact_right(real, other)
        + dot_exact_right(imag, other_i)
    )
    packed = packed_ref[...].astype(F32)
    row, column = triangle(packed.shape[0])
    upper = jnp.where(row <= column, packed, 0.0).astype(BF16)
    strict = jnp.where(row < column, packed, 0.0).astype(BF16)
    lower = jnp.where(row > column, packed, 0.0).astype(BF16)
    base_other_ref[...] = (
        dot(upper, other)
        + dot(strict, other, TN)
        + dot(lower, other_i)
        - dot(lower, other_i, TN)
        + dot_exact_right(real, own, TN)
        - dot_exact_right(imag, own_i, TN)
    )


def base(own, other, total, packed, mine):
    rows, width = own.shape
    return pl.pallas_call(
        base_kernel,
        in_specs=[VMEM] * 5,
        out_specs=[VMEM] * 2,
        out_shape=[jax.ShapeDtypeStruct((rows, width), F32)] * 2,
        cost_estimate=pl.CostEstimate(
            flops=32 * rows * rows * width, bytes_accessed=8 * rows * width, transcendentals=0
        ),
        name="base",
        compiler_params=LIMIT,
    )(own, other, total, packed, mine)


def update_kernel(scale, own_ref, other_ref, base_ref, base_other_ref, theirs_ref, out_ref, rows_ref):
    own, other = own_ref[...], other_ref[...]
    half = own.shape[1] // 2
    own_i, other_i = times_i(own.astype(F32)).astype(BF16), times_i(other.astype(F32)).astype(BF16)
    real, imag = theirs_ref[0], theirs_ref[1]
    rows = own.shape[0]
    product = base_ref[...] + dot(real, other) + dot(imag, other_i)
    rows_ref[:rows, :] = product
    rows_ref[rows:, :] = base_other_ref[...] + dot(real, own, TN) - dot(imag, own_i, TN)
    both = rows_ref[...].astype(BF16)
    blocks = dot(both, both, TN)
    real = blocks[:half, :half] + blocks[half:, half:]
    imag = blocks[:half, half:] - blocks[half:, :half]
    diagonal = lax.broadcasted_iota(jnp.int32, (half, 2 * half), 0) == lax.broadcasted_iota(
        jnp.int32, (half, 2 * half), 1
    )
    gram = jnp.concatenate([real, imag], axis=1)
    squares = jnp.sum(jnp.where(diagonal, gram, 0.0))
    size = jnp.full((1, 1), 2.0 * squares / half + 1e-06, F32)
    scaling = lax.rsqrt(size)
    rest = gram * (scaling * scaling) - jnp.where(diagonal, CENTRE, 0.0)
    square = 2.0 * CENTRE * rest + dot_complex(rest, rest)
    left_centre = 2.25 - 1.5 * CENTRE + 0.25 * CENTRE**2
    right_centre = 1.5 * CENTRE - 0.5 * CENTRE**2
    left = 0.25 * square - 1.5 * rest
    right = 1.5 * rest - 0.5 * square
    both_sides = left_centre * right + right_centre * left + dot_complex(left, right)
    factor = -0.75 * rest - 0.5 * both_sides
    centre = 2.25 - 0.75 * CENTRE - 0.5 * left_centre * right_centre
    stacked = jnp.concatenate([factor, times_i(factor)], axis=0)
    high, low = split(product)
    stacked_high, stacked_low = split(stacked)
    change = dot(high, stacked_high) + dot(low, stacked_high) + dot(high, stacked_low)
    out_ref[0] = (product * centre + change) * (scaling * scale)


def update(scale, own, other, bases, theirs):
    rows, width = own.shape
    return pl.pallas_call(
        functools.partial(update_kernel, scale),
        in_specs=[VMEM] * 5,
        out_specs=VMEM,
        out_shape=jax.ShapeDtypeStruct((1, rows, width), F32),
        scratch_shapes=[pltpu.VMEM((2 * rows, width), F32)],
        name="update",
        compiler_params=LIMIT,
    )(own, other, *bases, theirs)


def batch_shifts(batch, point_count):
    shifts = {}
    for member in range(BATCH):
        shift = displacement(SHELL_VECTORS[batch * BATCH + member], point_count)
        shifts.setdefault(shift, []).append(member)
    return shifts


def on_device(margins, subspace, shell_weights, window_count):
    point_count = lax.axis_size("kpt")
    side = lax.axis_index("band")
    rows = subspace.shape[1]
    swap = [(0, 1), (1, 0)]
    plan = [batch_shifts(batch, point_count) for batch in range(3)]

    def exchange(value):
        return lax.ppermute(value, "band", swap)

    def fetch(value, shift):
        return lax.ppermute(value, "kpt", fetch_pairs(shift, point_count))

    mark = prepare()
    place = (side[None], window_count.reshape(1, 1))
    own = subspace[0]
    other = exchange(own)
    margin = lax.dynamic_index_in_dim(margins[0], SHIPPED + 1 - side, 0, keepdims=False)
    margin = exchange(margin)
    halves = {}
    for part, value in (("own", own), ("other", other)):
        for batch in (2, 1):
            for shift in plan[batch]:
                halves[batch, part, shift] = fetch(value, shift)
        for shift in plan[0]:
            near = displacement((shift[0], 0, 1), point_count)
            step = displacement((0, shift[1], -1), point_count)
            halves[0, part, shift] = fetch(halves[1, part, near], step)

    def project_part(batch, members, extra, sent):
        groups, operands = [], []
        for shift, holders in plan[batch].items():
            group = [holder - members[0] for holder in holders if holder in members]
            if group:
                groups.append(group)
                operands += [halves[batch, "own", shift], halves[batch, "other", shift]]
        first = batch * BATCH + members[0]
        return project(place, shell_weights, margins, first, groups, operands, extra, sent)

    every = range(BATCH)
    blocks = {
        2: project_part(2, every, mark, True),
        1: project_part(1, every, mark, True),
        0: project_part(0, range(SHIPPED), mark, True),
    }
    *rest, got_extra = project_part(0, range(SHIPPED, BATCH), margin, False)
    got = {batch: exchange(blocks[batch][1]) for batch in (2, 1, 0)}
    (total,) = gather_own([*blocks[2], *blocks[1]], None)
    total, packed = gather_own([*blocks[0], *rest], total)
    other_packed = exchange(packed)
    whole = ((0, 0, 1, 0), (0, 1, 1, 1))
    crossed = cross([blocks[2][0], got[2]], whole, None, False)
    crossed = cross(
        [blocks[1][0], got[1], rest[0], got_extra], (*whole, (2, 0, 3, 0)), crossed, False
    )
    mine, theirs = cross([blocks[0][0], got[0]], ((0, 0, 1, 0),), crossed, True)
    theirs = exchange(theirs)
    bases = base(own, other, total, other_packed, mine)
    scale = math.sqrt(rows * lax.axis_size("band"))
    return update(scale, own, other, bases, theirs)


def solution(mesh):
    return jax.shard_map(
        on_device,
        mesh=mesh,
        in_specs=(P("kpt", None, "band", None), P("kpt", "band", None), P(), P("kpt")),
        out_specs=P("kpt", "band", None),
        check_vma=False,
    )
```

```python
import functools
import math

import jax
import jax.numpy as jnp
from jax import lax
from jax.experimental import pallas as pl
from jax.experimental.pallas import tpu as pltpu
from jax.sharding import PartitionSpec as P


SHELL_VECTORS = (
    (1, 1, 0),
    (1, -1, 0),
    (-1, 1, 0),
    (-1, -1, 0),
    (1, 0, 1),
    (1, 0, -1),
    (-1, 0, 1),
    (-1, 0, -1),
    (0, 1, 1),
    (0, 1, -1),
    (0, -1, 1),
    (0, -1, -1),
)
BATCH = 4
SHIPPED = 2
CENTRE = 0.5
LANES = 128
PREPARE = 2 * 10**10
VMEM = pl.BlockSpec(memory_space=pltpu.VMEM)
LIMIT = pltpu.CompilerParams(vmem_limit_bytes=20 * 2**20)
SMEM = pl.BlockSpec(memory_space=pltpu.SMEM)
F32 = jnp.float32
BF16 = jnp.bfloat16
NT = (((1,), (1,)), ((), ()))
TN = (((0,), (0,)), ((), ()))


def grid_shape(point_count):
    size_y = min(4, point_count // 8)
    return (4, size_y, point_count // (4 * size_y))


def displacement(shell, point_count):
    return tuple(step % size for step, size in zip(shell, grid_shape(point_count)))


def fetch_pairs(shift, point_count):
    size_x, size_y, size_z = grid_shape(point_count)
    pairs = []
    for x in range(size_x):
        for y in range(size_y):
            for z in range(size_z):
                source = ((x + shift[0]) % size_x, (y + shift[1]) % size_y, (z + shift[2]) % size_z)
                pairs.append(
                    (
                        (source[0] * size_y + source[1]) * size_z + source[2],
                        (x * size_y + y) * size_z + z,
                    )
                )
    return pairs


def dot(left, right, dims=None):
    if dims is None:
        return jnp.dot(left, right, preferred_element_type=F32)
    return lax.dot_general(left, right, dims, preferred_element_type=F32)


def split(value):
    high = value.astype(BF16)
    return high, (value - high.astype(F32)).astype(BF16)


def dot_exact_right(left, right, dims=None):
    high, low = split(left)
    return dot(high, right, dims) + dot(low, right, dims)


def times_minus_i(value):
    half = value.shape[-1] // 2
    return jnp.concatenate([value[:, half:], -value[:, :half]], axis=1)


def times_i(value):
    half = value.shape[-1] // 2
    return jnp.concatenate([-value[:, half:], value[:, :half]], axis=1)


def stack_complex(mine, other, side, rows_ref, stacked_ref):
    rows = mine.shape[0]
    rows_ref[pl.ds(pl.multiple_of(side * rows, 8), rows), :] = mine.astype(F32)
    rows_ref[pl.ds(pl.multiple_of((1 - side) * rows, 8), rows), :] = other.astype(F32)
    whole = rows_ref[...]
    stacked_ref[: 2 * rows, :] = whole.astype(BF16)
    stacked_ref[2 * rows :, :] = times_i(whole).astype(BF16)


def masked_blocks(margins, stacked, weights, limit):
    count, rows, double = margins.shape
    inside = lax.broadcasted_iota(jnp.int32, (rows, 1), 0) < limit
    products = dot(margins.reshape(count * rows, double), stacked)
    blocks = []
    for place, weight in enumerate(weights):
        factor = jnp.where(inside, jnp.sqrt(jnp.full((1, 1), weight, F32)), 0.0)
        blocks.append((products[place * rows : (place + 1) * rows] * factor).astype(BF16))
    return blocks


def prepare_kernel(out_ref):
    out_ref[...] = jnp.zeros_like(out_ref)


def prepare():
    return pl.pallas_call(
        prepare_kernel,
        out_specs=VMEM,
        out_shape=jax.ShapeDtypeStruct((8, 128), jnp.int32),
        cost_estimate=pl.CostEstimate(flops=PREPARE, bytes_accessed=2**26, transcendentals=0),
        name="prepare",
        compiler_params=LIMIT,
    )()


def project_kernel(groups, first, sent, side_ref, window_ref, weight_ref, margins_ref, *refs):
    halves = refs[: 2 * len(groups)]
    *out_refs, rows_ref, stacked_ref, blocks_ref = refs[2 * len(groups) :]
    shipped_ref = None
    if not sent:
        shipped_ref, keep_ref, other_ref, got_ref = out_refs
    else:
        _, keep_ref, other_ref = out_refs
    side = side_ref[0]
    rows = margins_ref.shape[2]
    limits = [window_ref[...] - side * rows, window_ref[...] - (1 - side) * rows]
    for number, members in enumerate(groups):
        mine, other = halves[2 * number][...], halves[2 * number + 1][...]
        stack_complex(mine, other, side, rows_ref, stacked_ref)
        start, count = first + members[0], len(members)
        blocks = masked_blocks(
            margins_ref[0, start : start + count],
            stacked_ref[...],
            [weight_ref[first + member] for member in members],
            limits[0],
        )
        for member, block in zip(members, blocks):
            blocks_ref[member] = block
            if not sent:
                @pl.when(side == member % 2)
                def _():
                    weight = weight_ref[first + member]
                    (got_ref[0],) = masked_blocks(
                        shipped_ref[...][None], stacked_ref[...], [weight], limits[1]
                    )
    for pair in range(keep_ref.shape[0]):
        keep_ref[pair] = blocks_ref[2 * pair + side]
        other_ref[pair] = blocks_ref[2 * pair + 1 - side]


def project(place, weights, margins, first, groups, halves, extra, sent):
    rows, double = margins.shape[2:]
    width = halves[0].shape[-1]
    members = sum(len(group) for group in groups)
    counts = [members // 2, members // 2] + ([] if sent else [1])
    return pl.pallas_call(
        functools.partial(project_kernel, groups, first, sent),
        in_specs=[SMEM, VMEM, SMEM, VMEM, *([VMEM] * len(halves)), VMEM],
        out_specs=[VMEM] * len(counts),
        out_shape=[jax.ShapeDtypeStruct((count, rows, width), BF16) for count in counts],
        scratch_shapes=[
            pltpu.VMEM((2 * rows, width), F32),
            pltpu.VMEM((double, width), BF16),
            pltpu.VMEM((members, rows, width), BF16),
        ],
        cost_estimate=pl.CostEstimate(
            flops=2 * members * rows * double * width,
            bytes_accessed=2 * members * rows * double,
            transcendentals=0,
        ),
        compiler_params=LIMIT,
    )(*place, weights, margins, *halves, extra)


def triangle(size):
    row = lax.broadcasted_iota(jnp.int32, (size, size), 0)
    return row, lax.broadcasted_iota(jnp.int32, (size, size), 1)


def gather_own_kernel(count, has_total, *refs):
    blocks, refs = refs[:count], refs[count:]
    rows = blocks[0].shape[1]
    real = jnp.zeros((rows, rows), F32)
    imag = jnp.zeros((rows, rows), F32)
    if has_total:
        real, imag = refs[0][0], refs[0][1]
    for block_ref in blocks:
        for pair in range(block_ref.shape[0]):
            block = block_ref[pair]
            real += dot(block, block, NT)
            imag += dot(times_minus_i(block), block, NT)
    total_ref, *packed = refs[1 if has_total else 0 :]
    total_ref[0], total_ref[1] = real, imag
    if packed:
        row, column = triangle(rows)
        packed[0][...] = jnp.where(row <= column, real, imag).astype(BF16)


def gather_own(blocks, before):
    rows, width = blocks[0].shape[1:]
    count = len(blocks)
    operands = list(blocks) + ([] if before is None else [before])
    results = [jax.ShapeDtypeStruct((2, rows, rows), F32)]
    if before is not None:
        results.append(jax.ShapeDtypeStruct((rows, rows), BF16))
    return pl.pallas_call(
        functools.partial(gather_own_kernel, count, before is not None),
        in_specs=[VMEM] * len(operands),
        out_specs=[VMEM] * len(results),
        out_shape=results,
        cost_estimate=pl.CostEstimate(
            flops=8 * count * rows * rows * width,
            bytes_accessed=4 * count * rows * width,
            transcendentals=0,
        ),
        compiler_params=LIMIT,
    )(*operands)


def packing(rows):
    even = rows // LANES * LANES
    left = rows - even
    fit = min(left, LANES - left)
    return even, left, fit, left - fit


def packed_shape(rows):
    even, _, _, spare = packing(rows)
    return (rows + -(-spare // 16) * 16, 2 * even + LANES)


def cross_kernel(terms, count, has_total, last, *refs):
    blocks, refs = refs[:count], refs[count:]
    rows = blocks[0].shape[1]
    sums = [jnp.zeros((rows, rows), F32) for _ in range(4)]
    if has_total:
        mine_before_ref, theirs_before_ref, *refs = refs
        sums = [mine_before_ref[0], mine_before_ref[1], theirs_before_ref[0], theirs_before_ref[1]]
    mine_ref, theirs_ref, *refs = refs
    for keep_place, keep_index, got_place, got_index in terms:
        keep, got = blocks[keep_place][keep_index], blocks[got_place][got_index]
        sums[0] += dot(keep, got, NT)
        sums[1] += dot(times_minus_i(keep), got, NT)
        sums[2] += dot(got, keep, NT)
        sums[3] += dot(times_minus_i(got), keep, NT)
    mine_ref[0], mine_ref[1] = sums[0], sums[1]
    real, imag = sums[2], sums[3]
    if not last:
        theirs_ref[0], theirs_ref[1] = real, imag
        return
    (packed_ref,) = refs
    even, left, fit, spare = packing(rows)
    packed_ref[:rows, :even] = real[:, :even]
    packed_ref[:rows, even : 2 * even] = imag[:, :even]
    packed_ref[:rows, 2 * even :] = jnp.concatenate(
        [
            real[:, even:],
            imag[:, even : even + fit],
            jnp.zeros((rows, LANES - left - fit), F32),
        ][: 3 if left + fit < LANES else 2],
        axis=1,
    )
    if spare:
        packed_ref[rows:, :] = jnp.zeros((packed_ref.shape[0] - rows, packed_ref.shape[1]), F32)
        row, column = triangle(rows)
        identity = jnp.where(row == column, 1.0, 0.0).astype(BF16)
        packed_ref[rows : rows + spare, :rows] = dot(
            imag[:, rows - spare :].astype(BF16), identity, TN
        )
    theirs_ref[...] = packed_ref[...].astype(BF16)


def cross(blocks, terms, before, last):
    rows, width = blocks[0].shape[1:]
    operands = [*blocks, *(before or ())]
    packed = packed_shape(rows)
    return pl.pallas_call(
        functools.partial(cross_kernel, terms, len(blocks), before is not None, last),
        in_specs=[VMEM] * len(operands),
        out_specs=[VMEM] * 2,
        out_shape=[
            jax.ShapeDtypeStruct((2, rows, rows), F32),
            jax.ShapeDtypeStruct(packed, BF16) if last else jax.ShapeDtypeStruct((2, rows, rows), F32),
        ],
        scratch_shapes=[pltpu.VMEM(packed, F32)] if last else [],
        cost_estimate=pl.CostEstimate(
            flops=8 * len(terms) * rows * rows * width,
            bytes_accessed=4 * len(terms) * rows * width,
            transcendentals=0,
        ),
        compiler_params=LIMIT,
    )(*operands)


def dot_complex(left, right):
    stacked = jnp.concatenate([right, times_i(right)], axis=0).astype(BF16)
    return dot(left.astype(BF16), stacked)


def base_kernel(
    own_ref, other_ref, total_ref, packed_ref, mine_ref, base_ref, base_other_ref, right_ref, stack_ref
):
    own, other = own_ref[...], other_ref[...]
    own_i, other_i = times_i(own.astype(F32)).astype(BF16), times_i(other.astype(F32)).astype(BF16)
    real, imag = mine_ref[0], mine_ref[1]
    base_ref[...] = (
        dot_exact_right(total_ref[0], own)
        + dot_exact_right(total_ref[1], own_i)
        + dot_exact_right(real, other)
        + dot_exact_right(imag, other_i)
    )
    packed = packed_ref[...].astype(F32)
    row, column = triangle(packed.shape[0])
    upper = jnp.where(row <= column, packed, 0.0).astype(BF16)
    strict = jnp.where(row < column, packed, 0.0).astype(BF16)
    lower = jnp.where(row > column, packed, 0.0).astype(BF16)
    base_other_ref[...] = (
        dot(upper, other)
        + dot(strict, other, TN)
        + dot(lower, other_i)
        - dot(lower, other_i, TN)
        + dot_exact_right(real, own, TN)
        - dot_exact_right(imag, own_i, TN)
    )
    even, left, fit, _ = packing(other.shape[0])
    plain, turned = other.astype(F32), times_i(other.astype(F32))
    stack_ref[:even, :] = plain[:even]
    stack_ref[even : 2 * even, :] = turned[:even]
    stack_ref[2 * even : 2 * even + left, :] = plain[even:]
    stack_ref[2 * even + left : 2 * even + left + fit, :] = turned[even : even + fit]
    if left + fit < LANES:
        stack_ref[2 * even + left + fit :, :] = jnp.zeros((LANES - left - fit, plain.shape[1]), F32)
    right_ref[...] = stack_ref[...].astype(BF16)


def base(own, other, total, packed, mine):
    rows, width = own.shape
    return pl.pallas_call(
        base_kernel,
        in_specs=[VMEM] * 5,
        out_specs=[VMEM] * 3,
        out_shape=[
            jax.ShapeDtypeStruct((rows, width), F32),
            jax.ShapeDtypeStruct((rows, width), F32),
            jax.ShapeDtypeStruct((packed_shape(rows)[1], width), BF16),
        ],
        scratch_shapes=[pltpu.VMEM((packed_shape(rows)[1], width), F32)],
        cost_estimate=pl.CostEstimate(
            flops=32 * rows * rows * width, bytes_accessed=8 * rows * width, transcendentals=0
        ),
        name="base",
        compiler_params=LIMIT,
    )(own, other, total, packed, mine)


def update_kernel(
    scale, own_ref, other_ref, base_ref, base_other_ref, right_ref, theirs_ref, out_ref, rows_ref
):
    own = own_ref[...]
    rows, half = own.shape[0], own.shape[1] // 2
    own_i = times_i(own.astype(F32)).astype(BF16)
    even, left, fit, spare = packing(rows)
    product = base_ref[...] + dot(theirs_ref[:rows, :], right_ref[...])
    upper = dot(theirs_ref[:rows, :even], own, TN) - dot(theirs_ref[:rows, even : 2 * even], own_i, TN)
    shared = theirs_ref[:rows, 2 * even :]
    lower = dot(shared, own, TN)[:left]
    turned = dot(shared, own_i, TN)[left : left + fit]
    if spare:
        below = theirs_ref[rows : rows + spare, :rows]
        other_i = times_i(other_ref[...].astype(F32)[rows - spare :]).astype(BF16)
        product += dot(below, other_i, TN)
        turned = jnp.concatenate([turned, dot(below, own_i)], axis=0)
    rows_ref[:rows, :] = product
    rows_ref[rows : rows + even, :] = base_other_ref[:even, :] + upper
    rows_ref[rows + even :, :] = base_other_ref[even:, :] + lower - turned
    both = rows_ref[...].astype(BF16)
    blocks = dot(both, both, TN)
    real = blocks[:half, :half] + blocks[half:, half:]
    imag = blocks[:half, half:] - blocks[half:, :half]
    diagonal = lax.broadcasted_iota(jnp.int32, (half, 2 * half), 0) == lax.broadcasted_iota(
        jnp.int32, (half, 2 * half), 1
    )
    gram = jnp.concatenate([real, imag], axis=1)
    squares = jnp.sum(jnp.where(diagonal, gram, 0.0))
    size = jnp.full((1, 1), 2.0 * squares / half + 1e-06, F32)
    scaling = lax.rsqrt(size)
    rest = gram * (scaling * scaling) - jnp.where(diagonal, CENTRE, 0.0)
    square = 2.0 * CENTRE * rest + dot_complex(rest, rest)
    left_centre = 2.25 - 1.5 * CENTRE + 0.25 * CENTRE**2
    right_centre = 1.5 * CENTRE - 0.5 * CENTRE**2
    left = 0.25 * square - 1.5 * rest
    right = 1.5 * rest - 0.5 * square
    both_sides = left_centre * right + right_centre * left + dot_complex(left, right)
    factor = -0.75 * rest - 0.5 * both_sides
    centre = 2.25 - 0.75 * CENTRE - 0.5 * left_centre * right_centre
    stacked = jnp.concatenate([factor, times_i(factor)], axis=0)
    high, low = split(product)
    stacked_high, stacked_low = split(stacked)
    change = dot(high, stacked_high) + dot(low, stacked_high) + dot(high, stacked_low)
    out_ref[0] = (product * centre + change) * (scaling * scale)


def update(scale, own, other, bases, theirs):
    rows, width = own.shape
    return pl.pallas_call(
        functools.partial(update_kernel, scale),
        in_specs=[VMEM] * 6,
        out_specs=VMEM,
        out_shape=jax.ShapeDtypeStruct((1, rows, width), F32),
        scratch_shapes=[pltpu.VMEM((2 * rows, width), F32)],
        name="update",
        compiler_params=LIMIT,
    )(own, other, *bases, theirs)


def batch_shifts(batch, point_count):
    shifts = {}
    for member in range(BATCH):
        shift = displacement(SHELL_VECTORS[batch * BATCH + member], point_count)
        shifts.setdefault(shift, []).append(member)
    return shifts


def on_device(margins, subspace, shell_weights, window_count):
    point_count = lax.axis_size("kpt")
    side = lax.axis_index("band")
    rows = subspace.shape[1]
    swap = [(0, 1), (1, 0)]
    plan = [batch_shifts(batch, point_count) for batch in range(3)]

    def exchange(value):
        return lax.ppermute(value, "band", swap)

    def fetch(value, shift):
        return lax.ppermute(value, "kpt", fetch_pairs(shift, point_count))

    mark = prepare()
    place = (side[None], window_count.reshape(1, 1))
    own = subspace[0]
    other = exchange(own)
    margin = lax.dynamic_index_in_dim(margins[0], SHIPPED + 1 - side, 0, keepdims=False)
    margin = exchange(margin)
    halves = {}
    for part, value in (("own", own), ("other", other)):
        for batch in (2, 1):
            for shift in plan[batch]:
                halves[batch, part, shift] = fetch(value, shift)
        for shift in plan[0]:
            near = displacement((shift[0], 0, 1), point_count)
            step = displacement((0, shift[1], -1), point_count)
            halves[0, part, shift] = fetch(halves[1, part, near], step)

    def project_part(batch, members, extra, sent):
        groups, operands = [], []
        for shift, holders in plan[batch].items():
            group = [holder - members[0] for holder in holders if holder in members]
            if group:
                groups.append(group)
                operands += [halves[batch, "own", shift], halves[batch, "other", shift]]
        first = batch * BATCH + members[0]
        return project(place, shell_weights, margins, first, groups, operands, extra, sent)

    every = range(BATCH)
    blocks = {
        2: project_part(2, every, mark, True),
        1: project_part(1, every, mark, True),
        0: project_part(0, range(SHIPPED), mark, True),
    }
    *rest, got_extra = project_part(0, range(SHIPPED, BATCH), margin, False)
    got = {batch: exchange(blocks[batch][1]) for batch in (2, 1, 0)}
    (total,) = gather_own([*blocks[2], *blocks[1]], None)
    total, packed = gather_own([*blocks[0], *rest], total)
    other_packed = exchange(packed)
    whole = ((0, 0, 1, 0), (0, 1, 1, 1))
    crossed = cross([blocks[2][0], got[2]], whole, None, False)
    crossed = cross(
        [blocks[1][0], got[1], rest[0], got_extra], (*whole, (2, 0, 3, 0)), crossed, False
    )
    mine, theirs = cross([blocks[0][0], got[0]], ((0, 0, 1, 0),), crossed, True)
    theirs = exchange(theirs)
    bases = base(own, other, total, other_packed, mine)
    scale = math.sqrt(rows * lax.axis_size("band"))
    return update(scale, own, other, bases, theirs)


def solution(mesh):
    return jax.shard_map(
        on_device,
        mesh=mesh,
        in_specs=(P("kpt", None, "band", None), P("kpt", "band", None), P(), P("kpt")),
        out_specs=P("kpt", "band", None),
        check_vma=False,
    )
```

```python
import functools
import math

import jax
import jax.numpy as jnp
from jax import lax
from jax.experimental import pallas as pl
from jax.experimental.pallas import tpu as pltpu
from jax.sharding import PartitionSpec as P


SHELL_VECTORS = (
    (1, 1, 0),
    (1, -1, 0),
    (-1, 1, 0),
    (-1, -1, 0),
    (1, 0, 1),
    (1, 0, -1),
    (-1, 0, 1),
    (-1, 0, -1),
    (0, 1, 1),
    (0, 1, -1),
    (0, -1, 1),
    (0, -1, -1),
)
BATCH = 4
SHIPPED = 2
CENTRE = 0.5
LANES = 128
PREPARE = 2 * 10**10
VMEM = pl.BlockSpec(memory_space=pltpu.VMEM)
LIMIT = pltpu.CompilerParams(vmem_limit_bytes=20 * 2**20)
SMEM = pl.BlockSpec(memory_space=pltpu.SMEM)
F32 = jnp.float32
BF16 = jnp.bfloat16
NT = (((1,), (1,)), ((), ()))
TN = (((0,), (0,)), ((), ()))


def grid_shape(point_count):
    size_y = min(4, point_count // 8)
    return (4, size_y, point_count // (4 * size_y))


def displacement(shell, point_count):
    return tuple(step % size for step, size in zip(shell, grid_shape(point_count)))


def fetch_pairs(shift, point_count):
    size_x, size_y, size_z = grid_shape(point_count)
    pairs = []
    for x in range(size_x):
        for y in range(size_y):
            for z in range(size_z):
                source = ((x + shift[0]) % size_x, (y + shift[1]) % size_y, (z + shift[2]) % size_z)
                pairs.append(
                    (
                        (source[0] * size_y + source[1]) * size_z + source[2],
                        (x * size_y + y) * size_z + z,
                    )
                )
    return pairs


def dot(left, right, dims=None):
    if dims is None:
        return jnp.dot(left, right, preferred_element_type=F32)
    return lax.dot_general(left, right, dims, preferred_element_type=F32)


def split(value):
    high = value.astype(BF16)
    return high, (value - high.astype(F32)).astype(BF16)


def dot_exact_right(left, right, dims=None):
    high, low = split(left)
    return dot(high, right, dims) + dot(low, right, dims)


def times_minus_i(value):
    half = value.shape[-1] // 2
    return jnp.concatenate([value[:, half:], -value[:, :half]], axis=1)


def times_i(value):
    half = value.shape[-1] // 2
    return jnp.concatenate([-value[:, half:], value[:, :half]], axis=1)


def stack_complex(mine, other, side, rows_ref, stacked_ref):
    rows = mine.shape[0]
    rows_ref[pl.ds(pl.multiple_of(side * rows, 8), rows), :] = mine.astype(F32)
    rows_ref[pl.ds(pl.multiple_of((1 - side) * rows, 8), rows), :] = other.astype(F32)
    whole = rows_ref[...]
    stacked_ref[: 2 * rows, :] = whole.astype(BF16)
    stacked_ref[2 * rows :, :] = times_i(whole).astype(BF16)


def masked(product, weight, limit):
    inside = lax.broadcasted_iota(jnp.int32, (product.shape[0], 1), 0) < limit
    return (product * jnp.where(inside, jnp.sqrt(jnp.full((1, 1), weight, F32)), 0.0)).astype(BF16)


def masked_blocks(margins, stacked, weights, limit):
    count, rows, double = margins.shape
    products = dot(margins.reshape(count * rows, double), stacked)
    return [
        masked(products[place * rows : (place + 1) * rows], weight, limit)
        for place, weight in enumerate(weights)
    ]


def prepare_kernel(out_ref):
    out_ref[...] = jnp.zeros_like(out_ref)


def prepare():
    return pl.pallas_call(
        prepare_kernel,
        out_specs=VMEM,
        out_shape=jax.ShapeDtypeStruct((8, 128), jnp.int32),
        cost_estimate=pl.CostEstimate(flops=PREPARE, bytes_accessed=2**26, transcendentals=0),
        name="prepare",
        compiler_params=LIMIT,
    )()


def project_kernel(groups, first, sent, side_ref, window_ref, weight_ref, margins_ref, *refs):
    halves = refs[: 2 * len(groups)]
    *out_refs, rows_ref, stacked_ref, blocks_ref = refs[2 * len(groups) :]
    shipped_ref = None
    if not sent:
        shipped_ref, keep_ref, other_ref, got_ref = out_refs
    else:
        _, keep_ref, other_ref = out_refs
    side = side_ref[0]
    rows = margins_ref.shape[2]
    limits = [window_ref[...] - side * rows, window_ref[...] - (1 - side) * rows]
    paired = []
    for number, members in enumerate(groups):
        mine, other = halves[2 * number][...], halves[2 * number + 1][...]
        stack_complex(mine, other, side, rows_ref, stacked_ref)
        if members[0] % 2 == 0 and len(members) % 2 == 0:
            for pair in range(members[0] // 2, members[-1] // 2 + 1):
                for out_ref, place in ((keep_ref, side), (other_ref, 1 - side)):
                    place = first + 2 * pair + place
                    product = dot(margins_ref[0, place], stacked_ref[...])
                    out_ref[pair] = masked(product, weight_ref[place], limits[0])
                paired.append(pair)
            if not sent:
                product = dot(shipped_ref[...], stacked_ref[...])
                got_ref[0] = masked(product, weight_ref[first + side], limits[1])
            continue
        start, count = first + members[0], len(members)
        blocks = masked_blocks(
            margins_ref[0, start : start + count],
            stacked_ref[...],
            [weight_ref[first + member] for member in members],
            limits[0],
        )
        for member, block in zip(members, blocks):
            blocks_ref[member] = block
            if not sent:
                @pl.when(side == member % 2)
                def _():
                    weight = weight_ref[first + member]
                    (got_ref[0],) = masked_blocks(
                        shipped_ref[...][None], stacked_ref[...], [weight], limits[1]
                    )
    for pair in [pair for pair in range(keep_ref.shape[0]) if pair not in paired]:
        keep_ref[pair] = blocks_ref[2 * pair + side]
        other_ref[pair] = blocks_ref[2 * pair + 1 - side]


def project(place, weights, margins, first, groups, halves, extra, sent):
    rows, double = margins.shape[2:]
    width = halves[0].shape[-1]
    members = sum(len(group) for group in groups)
    counts = [members // 2, members // 2] + ([] if sent else [1])
    return pl.pallas_call(
        functools.partial(project_kernel, groups, first, sent),
        in_specs=[SMEM, VMEM, SMEM, VMEM, *([VMEM] * len(halves)), VMEM],
        out_specs=[VMEM] * len(counts),
        out_shape=[jax.ShapeDtypeStruct((count, rows, width), BF16) for count in counts],
        scratch_shapes=[
            pltpu.VMEM((2 * rows, width), F32),
            pltpu.VMEM((double, width), BF16),
            pltpu.VMEM((members, rows, width), BF16),
        ],
        cost_estimate=pl.CostEstimate(
            flops=2 * members * rows * double * width,
            bytes_accessed=2 * members * rows * double,
            transcendentals=0,
        ),
        compiler_params=LIMIT,
    )(*place, weights, margins, *halves, extra)


def triangle(size):
    row = lax.broadcasted_iota(jnp.int32, (size, size), 0)
    return row, lax.broadcasted_iota(jnp.int32, (size, size), 1)


def gather_own_kernel(count, has_total, *refs):
    blocks, refs = refs[:count], refs[count:]
    rows = blocks[0].shape[1]
    real = jnp.zeros((rows, rows), F32)
    imag = jnp.zeros((rows, rows), F32)
    if has_total:
        real, imag = refs[0][0], refs[0][1]
    for block_ref in blocks:
        for pair in range(block_ref.shape[0]):
            block = block_ref[pair]
            real += dot(block, block, NT)
            imag += dot(times_minus_i(block), block, NT)
    total_ref, *packed = refs[1 if has_total else 0 :]
    total_ref[0], total_ref[1] = real, imag
    if packed:
        row, column = triangle(rows)
        packed[0][...] = jnp.where(row <= column, real, imag).astype(BF16)


def gather_own(blocks, before):
    rows, width = blocks[0].shape[1:]
    count = len(blocks)
    operands = list(blocks) + ([] if before is None else [before])
    results = [jax.ShapeDtypeStruct((2, rows, rows), F32)]
    if before is not None:
        results.append(jax.ShapeDtypeStruct((rows, rows), BF16))
    return pl.pallas_call(
        functools.partial(gather_own_kernel, count, before is not None),
        in_specs=[VMEM] * len(operands),
        out_specs=[VMEM] * len(results),
        out_shape=results,
        cost_estimate=pl.CostEstimate(
            flops=8 * count * rows * rows * width,
            bytes_accessed=4 * count * rows * width,
            transcendentals=0,
        ),
        compiler_params=LIMIT,
    )(*operands)


def packing(rows):
    even = rows // LANES * LANES
    left = rows - even
    fit = min(left, LANES - left)
    return even, left, fit, left - fit


def packed_shape(rows):
    even, _, _, spare = packing(rows)
    return (rows + -(-spare // 16) * 16, 2 * even + LANES)


def tiles_of(plain, turned):
    even, left, fit, _ = packing(plain.shape[0])
    pieces = [plain[:even], turned[:even], plain[even:], turned[even : even + fit]]
    if left + fit < LANES:
        pieces.append(jnp.zeros((LANES - left - fit, plain.shape[1]), plain.dtype))
    return jnp.concatenate(pieces, axis=0)


def cross_kernel(terms, count, has_total, *refs):
    blocks, refs = refs[:count], refs[count:]
    rows = blocks[0].shape[1]
    *_, spare = packing(rows)
    mine_ref, theirs_ref, packed_ref = refs[-3:]
    real = imag = jnp.zeros((rows, rows), F32)
    theirs = jnp.zeros((rows, packed_ref.shape[1]), F32)
    below = jnp.zeros((spare, rows), F32)
    if has_total:
        mine_before_ref, theirs_before_ref = refs[:2]
        real, imag = mine_before_ref[0], mine_before_ref[1]
        theirs = theirs_before_ref[:rows, :]
        if spare:
            below = theirs_before_ref[rows : rows + spare, :rows]
    for keep_place, keep_index, got_place, got_index in terms:
        keep, got = blocks[keep_place][keep_index], blocks[got_place][got_index]
        real += dot(keep, got, NT)
        imag += dot(times_minus_i(keep), got, NT)
        plain = keep.astype(F32)
        turned = times_i(plain)
        theirs += dot(got, tiles_of(plain, turned).astype(BF16), NT)
        if spare:
            below += dot(turned[rows - spare :].astype(BF16), got, NT)
    mine_ref[0], mine_ref[1] = real, imag
    packed_ref[:rows, :] = theirs
    if spare:
        packed_ref[rows:, :] = jnp.zeros((packed_ref.shape[0] - rows, packed_ref.shape[1]), F32)
        packed_ref[rows : rows + spare, :rows] = below
    theirs_ref[...] = packed_ref[...].astype(theirs_ref.dtype)


def cross(blocks, terms, before, last):
    rows, width = blocks[0].shape[1:]
    operands = [*blocks, *(before or ())]
    packed = packed_shape(rows)
    return pl.pallas_call(
        functools.partial(cross_kernel, terms, len(blocks), before is not None),
        in_specs=[VMEM] * len(operands),
        out_specs=[VMEM] * 2,
        out_shape=[
            jax.ShapeDtypeStruct((2, rows, rows), F32),
            jax.ShapeDtypeStruct(packed, BF16 if last else F32),
        ],
        scratch_shapes=[pltpu.VMEM(packed, F32)],
        cost_estimate=pl.CostEstimate(
            flops=8 * len(terms) * rows * rows * width,
            bytes_accessed=4 * len(terms) * rows * width,
            transcendentals=0,
        ),
        compiler_params=LIMIT,
    )(*operands)


def dot_complex(left, right):
    stacked = jnp.concatenate([right, times_i(right)], axis=0).astype(BF16)
    return dot(left.astype(BF16), stacked)


def base_kernel(
    own_ref, other_ref, total_ref, packed_ref, mine_ref, base_ref, base_other_ref, right_ref
):
    own, other = own_ref[...], other_ref[...]
    own_i, other_i = times_i(own.astype(F32)).astype(BF16), times_i(other.astype(F32)).astype(BF16)
    real, imag = mine_ref[0], mine_ref[1]
    base_ref[...] = (
        dot_exact_right(total_ref[0], own)
        + dot_exact_right(total_ref[1], own_i)
        + dot_exact_right(real, other)
        + dot_exact_right(imag, other_i)
    )
    packed = packed_ref[...].astype(F32)
    row, column = triangle(packed.shape[0])
    upper = jnp.where(row <= column, packed, 0.0).astype(BF16)
    strict = jnp.where(row < column, packed, 0.0).astype(BF16)
    lower = jnp.where(row > column, packed, 0.0).astype(BF16)
    base_other_ref[...] = (
        dot(upper, other)
        + dot(strict, other, TN)
        + dot(lower, other_i)
        - dot(lower, other_i, TN)
        + dot_exact_right(real, own, TN)
        - dot_exact_right(imag, own_i, TN)
    )
    plain = other.astype(F32)
    right_ref[...] = tiles_of(plain, times_i(plain)).astype(BF16)


def base(own, other, total, packed, mine):
    rows, width = own.shape
    return pl.pallas_call(
        base_kernel,
        in_specs=[VMEM] * 5,
        out_specs=[VMEM] * 3,
        out_shape=[
            jax.ShapeDtypeStruct((rows, width), F32),
            jax.ShapeDtypeStruct((rows, width), F32),
            jax.ShapeDtypeStruct((packed_shape(rows)[1], width), BF16),
        ],
        cost_estimate=pl.CostEstimate(
            flops=32 * rows * rows * width, bytes_accessed=8 * rows * width, transcendentals=0
        ),
        name="base",
        compiler_params=LIMIT,
    )(own, other, total, packed, mine)


def update_kernel(
    scale, own_ref, other_ref, base_ref, base_other_ref, right_ref, theirs_ref, out_ref, rows_ref
):
    own = own_ref[...]
    rows, half = own.shape[0], own.shape[1] // 2
    own_i = times_i(own.astype(F32)).astype(BF16)
    even, left, fit, spare = packing(rows)
    product = base_ref[...] + dot(theirs_ref[:rows, :], right_ref[...])
    upper = dot(theirs_ref[:rows, :even], own, TN) - dot(theirs_ref[:rows, even : 2 * even], own_i, TN)
    shared = theirs_ref[:rows, 2 * even :]
    lower = dot(shared, own, TN)[:left]
    turned = dot(shared, own_i, TN)[left : left + fit]
    if spare:
        below = theirs_ref[rows : rows + spare, :rows]
        other_i = times_i(other_ref[...].astype(F32)[rows - spare :]).astype(BF16)
        product += dot(below, other_i, TN)
        turned = jnp.concatenate([turned, dot(below, own_i)], axis=0)
    rows_ref[:rows, :] = product
    rows_ref[rows : rows + even, :] = base_other_ref[:even, :] + upper
    rows_ref[rows + even :, :] = base_other_ref[even:, :] + lower - turned
    both = rows_ref[...].astype(BF16)
    blocks = dot(both, both, TN)
    real = blocks[:half, :half] + blocks[half:, half:]
    imag = blocks[:half, half:] - blocks[half:, :half]
    diagonal = lax.broadcasted_iota(jnp.int32, (half, 2 * half), 0) == lax.broadcasted_iota(
        jnp.int32, (half, 2 * half), 1
    )
    gram = jnp.concatenate([real, imag], axis=1)
    squares = jnp.sum(rows_ref[...] * rows_ref[...])
    size = jnp.full((1, 1), 2.0 * squares / half + 1e-06, F32)
    scaling = lax.rsqrt(size)
    rest = gram * (scaling * scaling) - jnp.where(diagonal, CENTRE, 0.0)
    square = 2.0 * CENTRE * rest + dot_complex(rest, rest)
    left_centre = 2.25 - 1.5 * CENTRE + 0.25 * CENTRE**2
    right_centre = 1.5 * CENTRE - 0.5 * CENTRE**2
    left = 0.25 * square - 1.5 * rest
    right = 1.5 * rest - 0.5 * square
    both_sides = left_centre * right + right_centre * left + dot_complex(left, right)
    factor = -0.75 * rest - 0.5 * both_sides
    centre = 2.25 - 0.75 * CENTRE - 0.5 * left_centre * right_centre
    stacked = jnp.concatenate([factor, times_i(factor)], axis=0)
    high, low = split(product)
    stacked_high, stacked_low = split(stacked)
    change = dot(high, stacked_high) + dot(low, stacked_high) + dot(high, stacked_low)
    out_ref[0] = (product * centre + change) * (scaling * scale)


def update(scale, own, other, bases, theirs):
    rows, width = own.shape
    return pl.pallas_call(
        functools.partial(update_kernel, scale),
        in_specs=[VMEM] * 6,
        out_specs=VMEM,
        out_shape=jax.ShapeDtypeStruct((1, rows, width), F32),
        scratch_shapes=[pltpu.VMEM((2 * rows, width), F32)],
        name="update",
        compiler_params=LIMIT,
    )(own, other, *bases, theirs)


def batch_shifts(batch, point_count):
    shifts = {}
    for member in range(BATCH):
        shift = displacement(SHELL_VECTORS[batch * BATCH + member], point_count)
        shifts.setdefault(shift, []).append(member)
    return shifts


def on_device(margins, subspace, shell_weights, window_count):
    point_count = lax.axis_size("kpt")
    side = lax.axis_index("band")
    rows = subspace.shape[1]
    swap = [(0, 1), (1, 0)]
    plan = [batch_shifts(batch, point_count) for batch in range(3)]

    def exchange(value):
        return lax.ppermute(value, "band", swap)

    def fetch(value, shift):
        return lax.ppermute(value, "kpt", fetch_pairs(shift, point_count))

    mark = prepare()
    place = (side[None], window_count.reshape(1, 1))
    own = subspace[0]
    other = exchange(own)
    margin = lax.dynamic_index_in_dim(margins[0], SHIPPED + 1 - side, 0, keepdims=False)
    margin = exchange(margin)
    halves = {}
    for part, value in (("own", own), ("other", other)):
        for batch in (2, 1):
            for shift in plan[batch]:
                halves[batch, part, shift] = fetch(value, shift)
        for shift in plan[0]:
            near = displacement((shift[0], 0, 1), point_count)
            step = displacement((0, shift[1], -1), point_count)
            halves[0, part, shift] = fetch(halves[1, part, near], step)

    def project_part(batch, members, extra, sent):
        groups, operands = [], []
        for shift, holders in plan[batch].items():
            group = [holder - members[0] for holder in holders if holder in members]
            if group:
                groups.append(group)
                operands += [halves[batch, "own", shift], halves[batch, "other", shift]]
        first = batch * BATCH + members[0]
        return project(place, shell_weights, margins, first, groups, operands, extra, sent)

    every = range(BATCH)
    blocks = {
        2: project_part(2, every, mark, True),
        1: project_part(1, every, mark, True),
        0: project_part(0, range(SHIPPED), mark, True),
    }
    *rest, got_extra = project_part(0, range(SHIPPED, BATCH), margin, False)
    got = {batch: exchange(blocks[batch][1]) for batch in (2, 1, 0)}
    (total,) = gather_own([*blocks[2], *blocks[1], *blocks[0]], None)
    total, packed = gather_own(rest, total)
    other_packed = exchange(packed)
    whole = ((0, 0, 1, 0), (0, 1, 1, 1))
    crossed = cross([blocks[2][0], got[2]], whole, None, False)
    crossed = cross(
        [blocks[1][0], got[1], rest[0], got_extra], (*whole, (2, 0, 3, 0)), crossed, False
    )
    mine, theirs = cross([blocks[0][0], got[0]], ((0, 0, 1, 0),), crossed, True)
    theirs = exchange(theirs)
    bases = base(own, other, total, other_packed, mine)
    scale = math.sqrt(rows * lax.axis_size("band"))
    return update(scale, own, other, bases, theirs)


def solution(mesh):
    return jax.shard_map(
        on_device,
        mesh=mesh,
        in_specs=(P("kpt", None, "band", None), P("kpt", "band", None), P(), P("kpt")),
        out_specs=P("kpt", "band", None),
        check_vma=False,
    )
```

```python
import functools
import math

import jax
import jax.numpy as jnp
from jax import lax
from jax.experimental import pallas as pl
from jax.experimental.pallas import tpu as pltpu
from jax.sharding import PartitionSpec as P


SHELL_VECTORS = (
    (1, 1, 0),
    (1, -1, 0),
    (-1, 1, 0),
    (-1, -1, 0),
    (1, 0, 1),
    (1, 0, -1),
    (-1, 0, 1),
    (-1, 0, -1),
    (0, 1, 1),
    (0, 1, -1),
    (0, -1, 1),
    (0, -1, -1),
)
BATCH = 4
SHIPPED = 2
CENTRE = 0.5
LANES = 128
PREPARE = 2 * 10**10
VMEM = pl.BlockSpec(memory_space=pltpu.VMEM)
LIMIT = pltpu.CompilerParams(vmem_limit_bytes=20 * 2**20)
SMEM = pl.BlockSpec(memory_space=pltpu.SMEM)
F32 = jnp.float32
BF16 = jnp.bfloat16
NT = (((1,), (1,)), ((), ()))
TN = (((0,), (0,)), ((), ()))


def grid_shape(point_count):
    size_y = min(4, point_count // 8)
    return (4, size_y, point_count // (4 * size_y))


def displacement(shell, point_count):
    return tuple(step % size for step, size in zip(shell, grid_shape(point_count)))


def fetch_pairs(shift, point_count):
    size_x, size_y, size_z = grid_shape(point_count)
    pairs = []
    for x in range(size_x):
        for y in range(size_y):
            for z in range(size_z):
                source = ((x + shift[0]) % size_x, (y + shift[1]) % size_y, (z + shift[2]) % size_z)
                pairs.append(
                    (
                        (source[0] * size_y + source[1]) * size_z + source[2],
                        (x * size_y + y) * size_z + z,
                    )
                )
    return pairs


def dot(left, right, dims=None):
    if dims is None:
        return jnp.dot(left, right, preferred_element_type=F32)
    return lax.dot_general(left, right, dims, preferred_element_type=F32)


def split(value):
    high = value.astype(BF16)
    return high, (value - high.astype(F32)).astype(BF16)


def dot_exact_right(left, right, dims=None):
    high, low = split(left)
    return dot(high, right, dims) + dot(low, right, dims)


def times_minus_i(value):
    half = value.shape[-1] // 2
    return jnp.concatenate([value[:, half:], -value[:, :half]], axis=1)


def times_i(value):
    half = value.shape[-1] // 2
    return jnp.concatenate([-value[:, half:], value[:, :half]], axis=1)


def stack_complex(mine, other, side, rows_ref, stacked_ref):
    rows = mine.shape[0]
    rows_ref[pl.ds(pl.multiple_of(side * rows, 8), rows), :] = mine.astype(F32)
    rows_ref[pl.ds(pl.multiple_of((1 - side) * rows, 8), rows), :] = other.astype(F32)
    whole = rows_ref[...]
    stacked_ref[: 2 * rows, :] = whole.astype(BF16)
    stacked_ref[2 * rows :, :] = times_i(whole).astype(BF16)


def masked_blocks(margins, stacked, weights, limit):
    count, rows, double = margins.shape
    inside = lax.broadcasted_iota(jnp.int32, (rows, 1), 0) < limit
    products = dot(margins.reshape(count * rows, double), stacked)
    blocks = []
    for place, weight in enumerate(weights):
        factor = jnp.where(inside, jnp.sqrt(jnp.full((1, 1), weight, F32)), 0.0)
        blocks.append((products[place * rows : (place + 1) * rows] * factor).astype(BF16))
    return blocks


def prepare_kernel(out_ref):
    out_ref[...] = jnp.zeros_like(out_ref)


def prepare():
    return pl.pallas_call(
        prepare_kernel,
        out_specs=VMEM,
        out_shape=jax.ShapeDtypeStruct((8, 128), jnp.int32),
        cost_estimate=pl.CostEstimate(flops=PREPARE, bytes_accessed=2**26, transcendentals=0),
        name="prepare",
        compiler_params=LIMIT,
    )()


def project_kernel(groups, first, sent, side_ref, window_ref, weight_ref, margins_ref, *refs):
    halves = refs[: 2 * len(groups)]
    *out_refs, rows_ref, stacked_ref, blocks_ref = refs[2 * len(groups) :]
    shipped_ref = None
    if not sent:
        shipped_ref, keep_ref, other_ref, got_ref = out_refs
    else:
        _, keep_ref, other_ref = out_refs
    side = side_ref[0]
    rows = margins_ref.shape[2]
    limits = [window_ref[...] - side * rows, window_ref[...] - (1 - side) * rows]
    for number, members in enumerate(groups):
        mine, other = halves[2 * number][...], halves[2 * number + 1][...]
        stack_complex(mine, other, side, rows_ref, stacked_ref)
        start, count = first + members[0], len(members)
        blocks = masked_blocks(
            margins_ref[0, start : start + count],
            stacked_ref[...],
            [weight_ref[first + member] for member in members],
            limits[0],
        )
        for member, block in zip(members, blocks):
            blocks_ref[member] = block
            if not sent:
                @pl.when(side == member % 2)
                def _():
                    weight = weight_ref[first + member]
                    (got_ref[0],) = masked_blocks(
                        shipped_ref[...][None], stacked_ref[...], [weight], limits[1]
                    )
    for pair in range(keep_ref.shape[0]):
        keep_ref[pair] = blocks_ref[2 * pair + side]
        other_ref[pair] = blocks_ref[2 * pair + 1 - side]


def project(place, weights, margins, first, groups, halves, extra, sent):
    rows, double = margins.shape[2:]
    width = halves[0].shape[-1]
    members = sum(len(group) for group in groups)
    counts = [members // 2, members // 2] + ([] if sent else [1])
    return pl.pallas_call(
        functools.partial(project_kernel, groups, first, sent),
        in_specs=[SMEM, VMEM, SMEM, VMEM, *([VMEM] * len(halves)), VMEM],
        out_specs=[VMEM] * len(counts),
        out_shape=[jax.ShapeDtypeStruct((count, rows, width), BF16) for count in counts],
        scratch_shapes=[
            pltpu.VMEM((2 * rows, width), F32),
            pltpu.VMEM((double, width), BF16),
            pltpu.VMEM((members, rows, width), BF16),
        ],
        cost_estimate=pl.CostEstimate(
            flops=2 * members * rows * double * width,
            bytes_accessed=2 * members * rows * double,
            transcendentals=0,
        ),
        compiler_params=LIMIT,
    )(*place, weights, margins, *halves, extra)


def triangle(size):
    row = lax.broadcasted_iota(jnp.int32, (size, size), 0)
    return row, lax.broadcasted_iota(jnp.int32, (size, size), 1)


def gather_own_kernel(count, has_total, *refs):
    blocks, refs = refs[:count], refs[count:]
    rows = blocks[0].shape[1]
    real = jnp.zeros((rows, rows), F32)
    imag = jnp.zeros((rows, rows), F32)
    if has_total:
        real, imag = refs[0][0], refs[0][1]
    for block_ref in blocks:
        for pair in range(block_ref.shape[0]):
            block = block_ref[pair]
            real += dot(block, block, NT)
            imag += dot(times_minus_i(block), block, NT)
    total_ref, *packed = refs[1 if has_total else 0 :]
    total_ref[0], total_ref[1] = real, imag
    if packed:
        row, column = triangle(rows)
        packed[0][...] = jnp.where(row <= column, real, imag).astype(BF16)


def gather_own(blocks, before):
    rows, width = blocks[0].shape[1:]
    count = len(blocks)
    operands = list(blocks) + ([] if before is None else [before])
    results = [jax.ShapeDtypeStruct((2, rows, rows), F32)]
    if before is not None:
        results.append(jax.ShapeDtypeStruct((rows, rows), BF16))
    return pl.pallas_call(
        functools.partial(gather_own_kernel, count, before is not None),
        in_specs=[VMEM] * len(operands),
        out_specs=[VMEM] * len(results),
        out_shape=results,
        cost_estimate=pl.CostEstimate(
            flops=8 * count * rows * rows * width,
            bytes_accessed=4 * count * rows * width,
            transcendentals=0,
        ),
        compiler_params=LIMIT,
    )(*operands)


def packing(rows):
    even = rows // LANES * LANES
    left = rows - even
    fit = min(left, LANES - left)
    return even, left, fit, left - fit


def packed_shape(rows):
    even, _, _, spare = packing(rows)
    return (rows + -(-spare // 16) * 16, 2 * even + LANES)


def tiles_of(plain, turned):
    even, left, fit, _ = packing(plain.shape[0])
    pieces = [plain[:even], turned[:even], plain[even:], turned[even : even + fit]]
    if left + fit < LANES:
        pieces.append(jnp.zeros((LANES - left - fit, plain.shape[1]), plain.dtype))
    return jnp.concatenate(pieces, axis=0)


def cross_kernel(terms, count, has_total, *refs):
    blocks, refs = refs[:count], refs[count:]
    rows = blocks[0].shape[1]
    *_, spare = packing(rows)
    mine_ref, theirs_ref, packed_ref = refs[-3:]
    real = imag = jnp.zeros((rows, rows), F32)
    theirs = jnp.zeros((rows, packed_ref.shape[1]), F32)
    below = jnp.zeros((spare, rows), F32)
    if has_total:
        mine_before_ref, theirs_before_ref = refs[:2]
        real, imag = mine_before_ref[0], mine_before_ref[1]
        theirs = theirs_before_ref[:rows, :]
        if spare:
            below = theirs_before_ref[rows : rows + spare, :rows]
    for keep_place, keep_index, got_place, got_index in terms:
        keep, got = blocks[keep_place][keep_index], blocks[got_place][got_index]
        real += dot(keep, got, NT)
        imag += dot(times_minus_i(keep), got, NT)
        plain = keep.astype(F32)
        turned = times_i(plain)
        theirs += dot(got, tiles_of(plain, turned).astype(BF16), NT)
        if spare:
            below += dot(turned[rows - spare :].astype(BF16), got, NT)
    mine_ref[0], mine_ref[1] = real, imag
    packed_ref[:rows, :] = theirs
    if spare:
        packed_ref[rows:, :] = jnp.zeros((packed_ref.shape[0] - rows, packed_ref.shape[1]), F32)
        packed_ref[rows : rows + spare, :rows] = below
    theirs_ref[...] = packed_ref[...].astype(theirs_ref.dtype)


def cross(blocks, terms, before, last):
    rows, width = blocks[0].shape[1:]
    operands = [*blocks, *(before or ())]
    packed = packed_shape(rows)
    return pl.pallas_call(
        functools.partial(cross_kernel, terms, len(blocks), before is not None),
        in_specs=[VMEM] * len(operands),
        out_specs=[VMEM] * 2,
        out_shape=[
            jax.ShapeDtypeStruct((2, rows, rows), F32),
            jax.ShapeDtypeStruct(packed, BF16 if last else F32),
        ],
        scratch_shapes=[pltpu.VMEM(packed, F32)],
        cost_estimate=pl.CostEstimate(
            flops=8 * len(terms) * rows * rows * width,
            bytes_accessed=4 * len(terms) * rows * width,
            transcendentals=0,
        ),
        compiler_params=LIMIT,
    )(*operands)


def dot_complex(left, right):
    stacked = jnp.concatenate([right, times_i(right)], axis=0).astype(BF16)
    return dot(left.astype(BF16), stacked)


def base_kernel(
    own_ref, other_ref, total_ref, packed_ref, mine_ref, base_ref, base_other_ref, right_ref
):
    own, other = own_ref[...], other_ref[...]
    own_i, other_i = times_i(own.astype(F32)).astype(BF16), times_i(other.astype(F32)).astype(BF16)
    real, imag = mine_ref[0], mine_ref[1]
    base_ref[...] = (
        dot_exact_right(total_ref[0], own)
        + dot_exact_right(total_ref[1], own_i)
        + dot_exact_right(real, other)
        + dot_exact_right(imag, other_i)
    )
    packed = packed_ref[...].astype(F32)
    row, column = triangle(packed.shape[0])
    upper = jnp.where(row <= column, packed, 0.0).astype(BF16)
    strict = jnp.where(row < column, packed, 0.0).astype(BF16)
    lower = jnp.where(row > column, packed, 0.0).astype(BF16)
    base_other_ref[...] = (
        dot(upper, other)
        + dot(strict, other, TN)
        + dot(lower, other_i)
        - dot(lower, other_i, TN)
        + dot_exact_right(real, own, TN)
        - dot_exact_right(imag, own_i, TN)
    )
    plain = other.astype(F32)
    right_ref[...] = tiles_of(plain, times_i(plain)).astype(BF16)


def base(own, other, total, packed, mine):
    rows, width = own.shape
    return pl.pallas_call(
        base_kernel,
        in_specs=[VMEM] * 5,
        out_specs=[VMEM] * 3,
        out_shape=[
            jax.ShapeDtypeStruct((rows, width), F32),
            jax.ShapeDtypeStruct((rows, width), F32),
            jax.ShapeDtypeStruct((packed_shape(rows)[1], width), BF16),
        ],
        cost_estimate=pl.CostEstimate(
            flops=32 * rows * rows * width, bytes_accessed=8 * rows * width, transcendentals=0
        ),
        name="base",
        compiler_params=LIMIT,
    )(own, other, total, packed, mine)


def update_kernel(
    scale, own_ref, other_ref, base_ref, base_other_ref, right_ref, theirs_ref, out_ref, rows_ref
):
    own = own_ref[...]
    rows, half = own.shape[0], own.shape[1] // 2
    own_i = times_i(own.astype(F32)).astype(BF16)
    even, left, fit, spare = packing(rows)
    product = base_ref[...] + dot(theirs_ref[:rows, :], right_ref[...])
    upper = dot(theirs_ref[:rows, :even], own, TN) - dot(theirs_ref[:rows, even : 2 * even], own_i, TN)
    shared = theirs_ref[:rows, 2 * even :]
    lower = dot(shared, own, TN)[:left]
    turned = dot(shared, own_i, TN)[left : left + fit]
    if spare:
        below = theirs_ref[rows : rows + spare, :rows]
        other_i = times_i(other_ref[...].astype(F32)[rows - spare :]).astype(BF16)
        product += dot(below, other_i, TN)
        turned = jnp.concatenate([turned, dot(below, own_i)], axis=0)
    rows_ref[:rows, :] = product
    rows_ref[rows : rows + even, :] = base_other_ref[:even, :] + upper
    rows_ref[rows + even :, :] = base_other_ref[even:, :] + lower - turned
    both = rows_ref[...].astype(BF16)
    blocks = dot(both, both, TN)
    real = blocks[:half, :half] + blocks[half:, half:]
    imag = blocks[:half, half:] - blocks[half:, :half]
    diagonal = lax.broadcasted_iota(jnp.int32, (half, 2 * half), 0) == lax.broadcasted_iota(
        jnp.int32, (half, 2 * half), 1
    )
    gram = jnp.concatenate([real, imag], axis=1)
    squares = jnp.sum(rows_ref[...] * rows_ref[...])
    size = jnp.full((1, 1), 2.0 * squares / half + 1e-06, F32)
    scaling = lax.rsqrt(size)
    rest = gram * (scaling * scaling) - jnp.where(diagonal, CENTRE, 0.0)
    square = 2.0 * CENTRE * rest + dot_complex(rest, rest)
    left_centre = 2.25 - 1.5 * CENTRE + 0.25 * CENTRE**2
    right_centre = 1.5 * CENTRE - 0.5 * CENTRE**2
    left = 0.25 * square - 1.5 * rest
    right = 1.5 * rest - 0.5 * square
    both_sides = left_centre * right + right_centre * left + dot_complex(left, right)
    factor = -0.75 * rest - 0.5 * both_sides
    centre = 2.25 - 0.75 * CENTRE - 0.5 * left_centre * right_centre
    stacked = jnp.concatenate([factor, times_i(factor)], axis=0)
    high, low = split(product)
    stacked_high, stacked_low = split(stacked)
    change = dot(high, stacked_high) + dot(low, stacked_high) + dot(high, stacked_low)
    out_ref[0] = (product * centre + change) * (scaling * scale)


def update(scale, own, other, bases, theirs):
    rows, width = own.shape
    return pl.pallas_call(
        functools.partial(update_kernel, scale),
        in_specs=[VMEM] * 6,
        out_specs=VMEM,
        out_shape=jax.ShapeDtypeStruct((1, rows, width), F32),
        scratch_shapes=[pltpu.VMEM((2 * rows, width), F32)],
        name="update",
        compiler_params=LIMIT,
    )(own, other, *bases, theirs)


def batch_shifts(batch, point_count):
    shifts = {}
    for member in range(BATCH):
        shift = displacement(SHELL_VECTORS[batch * BATCH + member], point_count)
        shifts.setdefault(shift, []).append(member)
    return shifts


def on_device(margins, subspace, shell_weights, window_count):
    point_count = lax.axis_size("kpt")
    side = lax.axis_index("band")
    rows = subspace.shape[1]
    swap = [(0, 1), (1, 0)]
    plan = [batch_shifts(batch, point_count) for batch in range(3)]

    def exchange(value):
        return lax.ppermute(value, "band", swap)

    def fetch(value, shift):
        return lax.ppermute(value, "kpt", fetch_pairs(shift, point_count))

    mark = prepare()
    place = (side[None], window_count.reshape(1, 1))
    own = subspace[0]
    other = exchange(own)
    margin = lax.dynamic_index_in_dim(margins[0], SHIPPED + 1 - side, 0, keepdims=False)
    margin = exchange(margin)
    halves = {}
    for part, value in (("own", own), ("other", other)):
        for batch in (2, 1):
            for shift in plan[batch]:
                halves[batch, part, shift] = fetch(value, shift)
        for shift in plan[0]:
            near = displacement((shift[0], 0, 1), point_count)
            step = displacement((0, shift[1], -1), point_count)
            halves[0, part, shift] = fetch(halves[1, part, near], step)

    def project_part(batch, members, extra, sent):
        groups, operands = [], []
        for shift, holders in plan[batch].items():
            group = [holder - members[0] for holder in holders if holder in members]
            if group:
                groups.append(group)
                operands += [halves[batch, "own", shift], halves[batch, "other", shift]]
        first = batch * BATCH + members[0]
        return project(place, shell_weights, margins, first, groups, operands, extra, sent)

    every = range(BATCH)
    blocks = {
        2: project_part(2, every, mark, True),
        1: project_part(1, every, mark, True),
        0: project_part(0, range(SHIPPED), mark, True),
    }
    *rest, got_extra = project_part(0, range(SHIPPED, BATCH), margin, False)
    got = {batch: exchange(blocks[batch][1]) for batch in (2, 1, 0)}
    (total,) = gather_own([*blocks[2], *blocks[1], *blocks[0]], None)
    total, packed = gather_own(rest, total)
    other_packed = exchange(packed)
    whole = ((0, 0, 1, 0), (0, 1, 1, 1))
    crossed = cross([blocks[2][0], got[2]], whole, None, False)
    crossed = cross(
        [blocks[1][0], got[1], rest[0], got_extra], (*whole, (2, 0, 3, 0)), crossed, False
    )
    mine, theirs = cross([blocks[0][0], got[0]], ((0, 0, 1, 0),), crossed, True)
    theirs = exchange(theirs)
    bases = base(own, other, total, other_packed, mine)
    scale = math.sqrt(rows * lax.axis_size("band"))
    return update(scale, own, other, bases, theirs)


def solution(mesh):
    return jax.shard_map(
        on_device,
        mesh=mesh,
        in_specs=(P("kpt", None, "band", None), P("kpt", "band", None), P(), P("kpt")),
        out_specs=P("kpt", "band", None),
        check_vma=False,
    )
```
